256 devices in a mesh: parts: 2 (over z), row: 128 (over y, x, core).
Axes of the slice: x: 8, y: 8, z: 2, core: 2. Of those that a mesh axis runs over, the one named last changes fastest.
The devices are a block of a 8x8x16 slice.
Arguments:
- sigma_top: bfloat16 [4096, 2048], P(('parts', 'row')), parts along dimension 0, may hold values from -2 to 8, as said below
- panel_par: bfloat16 [4096, 1024], P(('parts', 'row')), parts along dimension 0, may hold values from -0.25 to 0.25
- dinv_par: float32 [2048, 1024], P(('parts', 'row')), parts along dimension 0, may hold values from -2 to 8, as said below
- panel_kid_top: bfloat16 [4, 2048, 1024], P('parts', 'row'), parts along dimension 0, may hold values from -0.25 to 0.25
- panel_kid_par: bfloat16 [4, 1024, 1024], P('parts', 'row'), parts along dimension 0, may hold values from -0.375 to 0.375
- dvar_kid: float32 [4, 1024], P('parts'), parts along dimension 0, may hold values from 0.5 to 2
- mask_par: int32 [16, 4], P('parts'), parts along dimension 0, may hold values 0 or 1
- mask_kid_top: int32 [4, 8, 4], P('parts'), parts along dimension 0, may hold values 0 or 1
- mask_kid_par: int32 [4, 4, 4], P('parts'), parts along dimension 0, may hold values 0 or 1
Outputs:
- cross_par: bfloat16 [4096, 1024], P(('parts', 'row')), parts along dimension 0
- sigma_par: bfloat16 [2048, 1024], P(('parts', 'row')), parts along dimension 0
- cross_kid_top: bfloat16 [4, 2048, 1024], P('parts', 'row'), parts along dimension 0
- cross_kid_par: bfloat16 [4, 1024, 1024], P('parts', 'row'), parts along dimension 0
- variance_kid: float32 [4, 1024], P('parts'), parts along dimension 0
The draws below stay inside these ranges and needn't reach their ends.
There are 2 independent parts, one for each index of `parts`. The reference program is written for one: setup_inputs(seed, part) draws one part's arguments, and reference() takes and returns one part's arrays. A program takes and returns all parts, laid end to end along the dimension named above; each array names one. Nothing has to cross between parts.
Inputs may be any that keep to these rules, and one draw needn't show every extreme that they name: `sigma_top`: symmetric positive definite. `dinv_par`: symmetric positive definite.
All inputs are finite; a program needn't handle non-finite values.
Results may differ from the reference program's by a relative error of at most 0.0052.
Values may be sent and summed in bfloat16 or wider, within the bound.
No kernel may reach another device: no remote copies, remote signals or barrier semaphores. Data moves between devices by JAX's collectives and lax.ppermute only.
A program may use at most 64 MiB of HBM per device.

```python
import math
import jax
import jax.numpy as jnp
from jax import lax

WT = 2048
W1 = 1024
W2 = 1024
BLK = 256
KIDS = 2


def definite(key, width):
    first, second = jax.random.split(key, 2)
    raw = jax.random.normal(first, (width, width), jnp.float32)
    sym = (raw + raw.T) * (0.25 / jnp.sqrt(jnp.float32(width)))
    diag_part = jax.random.uniform(second, (width,), jnp.float32, 1.0, 2.0)
    whole = sym + jnp.diag(diag_part)
    return whole


def draw_sigma_top(key, part):
    return definite(jax.random.fold_in(key, 11), WT).astype(jnp.bfloat16)


def draw_dinv_par(key, part):
    return definite(jax.random.fold_in(key, 23), W1)


def place_ends(entries, key, low, high):
    longest = entries.shape.index(max(entries.shape))
    spots = []
    for shift in (0, 1):
        where = [jax.random.randint(jax.random.fold_in(key, axis), (), 0, length) for axis, length in enumerate(entries.shape)]
        where[longest] = (where[longest] + shift) % entries.shape[longest]
        spots.append(tuple(where))
    return entries.at[spots[0]].set(low).at[spots[1]].set(high)


def block_scale(rng, extent, shards, smallest, high):
    def one(position, parts):
        steps = jax.random.uniform(jax.random.fold_in(jax.random.fold_in(rng, 6), position), (parts,), jnp.float32, smallest / len(shards), high / len(shards))
        return jnp.repeat(jnp.exp(steps), extent[position] // parts).reshape((-1,) + (1,) * (len(extent) - position - 1))

    level = one(*shards[0])
    for cut in shards[1:]:
        level = level * one(*cut)
    return level


def noise(own_key, shape, spread, reach, cuts=(), dtype=jnp.bfloat16):
    entries = jax.random.normal(own_key, shape, jnp.float32) * spread
    if len(cuts) > 0:
        entries = block_scale(own_key, shape, cuts, -0.22, 0.18) * entries
    return jnp.clip(entries, min=-reach, max=reach).astype(dtype)


def setup_inputs(seed: int = 0, part: int = 0) -> dict:
    arg_keys = jax.random.split(jax.random.key(seed), 10)
    part_splits = jax.random.split(jax.random.fold_in(arg_keys[9], part), 10)
    return {
        "sigma_top": draw_sigma_top(jax.random.fold_in(jax.random.fold_in(arg_keys[9], part), 71), part),
        "panel_par": noise(part_splits[1], (WT, W1), (WT // 4) ** -0.5, 0.25, ((0, 128),)),
        "dinv_par": draw_dinv_par(jax.random.fold_in(jax.random.fold_in(arg_keys[9], part), 71), part),
        "panel_kid_top": noise(part_splits[3], (KIDS, WT, W2), (WT // 4) ** -0.5, 0.25, ((1, 128),)),
        "panel_kid_par": noise(part_splits[4], (KIDS, W1, W2), (W1 // 4) ** -0.5, 0.375, ((1, 128),)),
        "dvar_kid": jnp.clip(jnp.exp(jax.random.uniform(part_splits[5], (KIDS, W2), jnp.float32, math.log(0.5), math.log(2.0))), 0.5, 2.0),
        "mask_par": place_ends((jax.random.randint(part_splits[6], (WT // BLK, W1 // BLK), 0, 3) < 2).astype(jnp.int32), jax.random.fold_in(part_splits[6], 1), 0, 1),
        "mask_kid_top": place_ends((jax.random.randint(part_splits[7], (KIDS, WT // BLK, W2 // BLK), 0, 3) < 2).astype(jnp.int32), jax.random.fold_in(part_splits[7], 1), 0, 1),
        "mask_kid_par": place_ends((jax.random.randint(part_splits[8], (KIDS, W1 // BLK, W2 // BLK), 0, 3) < 2).astype(jnp.int32), jax.random.fold_in(part_splits[8], 1), 0, 1),
    }


def widen(mask):
    grown = jnp.repeat(jnp.repeat(mask, BLK, axis=-2), BLK, axis=-1)
    return grown.astype(jnp.bfloat16)


def reference(sigma_top, panel_par, dinv_par, panel_kid_top, panel_kid_par, dvar_kid, mask_par, mask_kid_top, mask_kid_par):
    high = lax.Precision.HIGHEST
    par_masked = panel_par * widen(mask_par)
    kid_top_masked = panel_kid_top * widen(mask_kid_top)
    kid_par_masked = panel_kid_par * widen(mask_kid_par)
    cross_par = jnp.dot(sigma_top, par_masked, preferred_element_type=jnp.float32).astype(jnp.bfloat16)
    sigma_par = (dinv_par + jnp.dot(par_masked.T, cross_par, preferred_element_type=jnp.float32)).astype(jnp.bfloat16)
    sig_wide = sigma_top.astype(jnp.float32)
    cross_wide = cross_par.astype(jnp.float32)
    spar_wide = sigma_par.astype(jnp.float32)
    ktop_wide = kid_top_masked.astype(jnp.float32)
    kpar_wide = kid_par_masked.astype(jnp.float32)
    kid_top = jnp.einsum("ac,kcw->kaw", sig_wide, ktop_wide, precision=high)
    kid_top = kid_top + jnp.einsum("ap,kpw->kaw", cross_wide, kpar_wide, precision=high)
    cross_kid_top = kid_top.astype(jnp.bfloat16)
    kid_par = jnp.einsum("ap,kaw->kpw", cross_wide, ktop_wide, precision=high)
    kid_par = kid_par + jnp.einsum("pq,kqw->kpw", spar_wide, kpar_wide, precision=high)
    cross_kid_par = kid_par.astype(jnp.bfloat16)
    variance_kid = dvar_kid + jnp.sum(ktop_wide * cross_kid_top.astype(jnp.float32), axis=1)
    variance_kid = variance_kid + jnp.sum(kpar_wide * cross_kid_par.astype(jnp.float32), axis=1)
    return cross_par, sigma_par, cross_kid_top, cross_kid_par, variance_kid
```

```python
import jax
import jax.numpy as jnp
from jax import lax
from jax.sharding import Mesh
from jax.sharding import PartitionSpec as P

BLK = 256
LANES = 128
ROW = ("y", "x", "c")
PARTS_ROW = ("parts", "y", "x", "c")
XC = ("x", "c")
F32 = jnp.float32
BF16 = jnp.bfloat16


def exchanged(x, axes):
    return lax.all_to_all(x, axes, split_axis=0, concat_axis=0, tiled=True)


def sent_to_all(x, axes):
    return exchanged(jnp.broadcast_to(x, (lax.axis_size(axes), *x.shape)), axes)


def row_mask(mask, rows, first):
    picked = lax.dynamic_index_in_dim(mask, first // BLK, axis=mask.ndim - 2, keepdims=True)
    assert BLK % rows == 0
    return jnp.repeat(picked, BLK, axis=-1).astype(BF16)


def dot(a, b):
    return jnp.dot(a, b, preferred_element_type=F32)


def dot_t(a, b):
    return lax.dot_general(a, b, (((0,), (0,)), ((), ())), preferred_element_type=F32)


def split3(v):
    parts = []
    for _ in range(3):
        top = lax.reduce_precision(v, 8, 7)
        parts.append(top.astype(BF16))
        v = v - top
    return jnp.stack(parts + [jnp.zeros_like(parts[0])])


def column_slots(x):
    rows = x.shape[-2]
    x = x.reshape(-1, rows, x.shape[-1] // LANES, LANES)
    return x.transpose(0, 2, 1, 3).reshape(-1, rows, LANES)


def from_column_slots(x, kids):
    rows = x.shape[1]
    x = x.reshape(kids, -1, rows, LANES).transpose(0, 2, 1, 3)
    return x.reshape(kids, rows, -1)


def halves_beside(x):
    n, rows, width = x.shape
    x = x.reshape(n, 2, rows // 2, width).transpose(0, 2, 1, 3)
    return x.reshape(n, rows // 2, 2 * width)


def halves_below(x):
    n, rows, width = x.shape
    x = x.reshape(n, rows, 2, width // 2).transpose(0, 2, 1, 3)
    return x.reshape(n, 2 * rows, width // 2)


def shards(
    sigma_top,
    panel_par,
    dinv_par,
    panel_kid_top,
    panel_kid_par,
    dvar_kid,
    mask_par,
    mask_kid_top,
    mask_kid_par,
):
    rt, wt = sigma_top.shape
    rp, w1 = dinv_par.shape
    kids, _, w2 = panel_kid_top.shape
    ny = lax.axis_size("y")
    nx = lax.axis_size("x")
    nj = lax.axis_size(XC)
    half = w1 // nj
    assert kids * w2 == nj * LANES and 2 * half == LANES and wt == 2 * w1
    position = lax.axis_index(ROW)
    first_core = lax.axis_index("c") == 0

    def in_order(own, other, rows):
        own = own.reshape(nx, rows, -1)
        other = other.reshape(nx, rows, -1)
        low = jnp.where(first_core, own, other)
        high = jnp.where(first_core, other, own)
        return jnp.stack([low, high], axis=1).reshape(nj, rows, -1)

    par = panel_par * row_mask(mask_par, rt, position * rt)
    kid_top = panel_kid_top * row_mask(mask_kid_top, rt, position * rt)
    kid_par = panel_kid_par * row_mask(mask_kid_par, rp, position * rp)

    par_slots = halves_beside(par.reshape(rt, nj, half).transpose(1, 0, 2))
    cols = jnp.concatenate([column_slots(kid_par), par_slots, column_slots(kid_top)], axis=1)
    cols = exchanged(cols, XC)
    rows = jnp.concatenate([par, sigma_top[:, :w1], sigma_top[:, w1:], dinv_par.astype(BF16)])
    rows = sent_to_all(rows, "x")
    others = lax.ppermute(rows, "c", [(0, 1), (1, 0)])

    def pieces(r):
        cut = [0, rt, 2 * rt, 3 * rt, 3 * rt + rp]
        return [r[:, a:b].reshape(-1, w1) for a, b in zip(cut[:-1], cut[1:])]

    par_own, s0_own, s1_own, d_own = pieces(rows)
    par_oth, s0_oth, s1_oth, d_oth = pieces(others)

    tall = sent_to_all(cols[:, : 2 * rp], "y")
    kid_par_j = tall[:, :, :rp].reshape(w1, LANES)
    par_j = halves_below(tall[:, :, rp:].reshape(ny * nj, rp, LANES)).reshape(wt, half)

    kid_par_tile = cols[:, :rp].astype(F32)
    kid_top_tile = cols[:, 2 * rp :].astype(F32)
    step = kid_top_tile + in_order(dot(par_own, kid_par_j), dot(par_oth, kid_par_j), rt)
    step_j = sent_to_all(step.astype(BF16), "y").reshape(wt, LANES)

    both_j = jnp.concatenate([step_j, par_j], axis=1)
    x_own = (dot(s0_own, both_j[:w1]) + dot(s1_own, both_j[w1:])).astype(BF16)
    x_oth = (dot(s0_oth, both_j[:w1]) + dot(s1_oth, both_j[w1:])).astype(BF16)
    x_tile = in_order(x_own, x_oth, rt)
    kt_tile = x_tile[:, :, :LANES]
    c_tile = x_tile[:, :, LANES:]

    db_tile = in_order(dot(d_own, kid_par_j), dot(d_oth, kid_par_j), rp)
    var_part = jnp.sum(step * kt_tile.astype(F32), axis=(0, 1))
    var_part = var_part + jnp.sum(kid_par_tile * db_tile, axis=(0, 1))

    y_part = dot_t(par_own, x_own) + dot_t(par_oth, x_oth)
    kp_part = y_part[:, :LANES].astype(BF16).reshape(ny, nj * rp, LANES)
    q_part = halves_beside(y_part[:, LANES:].astype(BF16).reshape(ny * nj, rp, half))
    q_part = q_part.reshape(ny, nj * rp // 2, LANES)
    var_rows = jnp.broadcast_to(split3(var_part), (ny, 4, LANES))
    summed = exchanged(jnp.concatenate([kp_part, q_part, var_rows], axis=1), "y")
    summed = jnp.sum(summed.astype(F32), axis=0)
    n1 = nj * rp
    kp_tile = summed[:n1].reshape(nj, rp, LANES) + db_tile
    q_tile = summed[n1 : n1 + n1 // 2].reshape(nj, rp // 2, LANES)
    var_j = jnp.sum(summed[n1 + n1 // 2 :], axis=0)

    out = jnp.concatenate(
        [
            kt_tile,
            kp_tile.astype(BF16),
            halves_beside(c_tile),
            q_tile.astype(BF16),
            jnp.broadcast_to(split3(var_j), (nj, 4, LANES)),
        ],
        axis=1,
    )
    out = exchanged(out, XC)
    cut = [rt, rt + rp, rt + 2 * rp, rt + 2 * rp + rp // 2]
    kt, kp, cr, q, var = jnp.split(out, cut, axis=1)
    cross_kid_top = from_column_slots(kt, kids)
    cross_kid_par = from_column_slots(kp, kids)
    cross_par = halves_below(cr).transpose(1, 0, 2).reshape(rt, w1)
    q = halves_below(q).transpose(1, 0, 2).reshape(rp, w1)
    sigma_par = (dinv_par + q.astype(F32)).astype(BF16)
    variance_kid = dvar_kid + jnp.sum(var.astype(F32), axis=1).reshape(kids, w2)
    return (cross_par, sigma_par, cross_kid_top, cross_kid_par, variance_kid)


def solution(mesh):
    finer = Mesh(mesh.devices.reshape(mesh.shape["parts"], 8, 8, 2), PARTS_ROW)
    return jax.shard_map(
        shards,
        mesh=finer,
        in_specs=(
            P(PARTS_ROW, None),
            P(PARTS_ROW, None),
            P(PARTS_ROW, None),
            P("parts", ROW, None),
            P("parts", ROW, None),
            P("parts", None),
            P("parts", None),
            P("parts", None, None),
            P("parts", None, None),
        ),
        out_specs=(
            P(PARTS_ROW, None),
            P(PARTS_ROW, None),
            P("parts", ROW, None),
            P("parts", ROW, None),
            P("parts", None),
        ),
        check_vma=False,
    )
```

```python
import jax
import jax.numpy as jnp
from jax import lax
from jax.experimental import pallas as pl
from jax.experimental.pallas import tpu as pltpu
from jax.sharding import Mesh
from jax.sharding import PartitionSpec as P

BLK = 256
LANES = 128
HALF = LANES // 2
ROW = ("y", "x", "c")
PARTS_ROW = ("parts", "y", "x", "c")
XC = ("x", "c")
F32 = jnp.float32
BF16 = jnp.bfloat16
VMEM = pl.BlockSpec(memory_space=pltpu.VMEM)
SMEM = pl.BlockSpec(memory_space=pltpu.SMEM)


def exchanged(x, axes):
    return lax.all_to_all(x, axes, split_axis=0, concat_axis=0, tiled=True)


def sent_to_all(x, axes):
    return exchanged(jnp.broadcast_to(x, (lax.axis_size(axes), *x.shape)), axes)


def swapped(x, axis, bit):
    return lax.ppermute(x, axis, [(i, i ^ bit) for i in range(lax.axis_size(axis))])


def dot(a, b):
    return jnp.dot(a, b, preferred_element_type=F32)


def dot_t(a, b):
    return lax.dot_general(a, b, (((0,), (0,)), ((), ())), preferred_element_type=F32)


def turned(x):
    return pltpu.roll(x, HALF, x.ndim - 1)


def low_high(low, high):
    lane = lax.broadcasted_iota(jnp.int32, low.shape, low.ndim - 1)
    return jnp.where(lane < HALF, low, high)


def split3(v):
    parts = []
    for _ in range(3):
        top = v.astype(BF16).astype(F32)
        parts.append(top)
        v = v - top
    return parts


def call(kernel, outs, args, specs=None, scratch=()):
    return pl.pallas_call(
        kernel,
        out_shape=tuple(jax.ShapeDtypeStruct(s, d) for s, d in outs),
        in_specs=specs or [VMEM] * len(args),
        out_specs=tuple(VMEM for _ in outs),
        scratch_shapes=scratch,
        compiler_params=pltpu.CompilerParams(vmem_limit_bytes=48 * 2**20),
    )(*args)


def pack_kernel(
    sigma, par, dinv, kid_top, kid_par, mask_par, mask_kid_top, mask_kid_par, slots, own
):
    rt, w1 = par.shape
    rp = dinv.shape[0]
    kids = kid_top.shape[0]
    nj = slots.shape[0]
    position = lax.axis_index(ROW)
    block_top = lax.div(position * rt, BLK)
    block_par = lax.div(position * rp, BLK)
    own[0:rt, :] = sigma[:, 0:w1]
    own[rt : 2 * rt, :] = sigma[:, w1 : 2 * w1]
    own[2 * rt : 2 * rt + rp, :] = dinv[...].astype(BF16)

    packed = []
    for m in range(w1 // LANES):
        at = slice(m * LANES, (m + 1) * LANES)
        keep = mask_par[block_top, m * LANES // BLK].astype(F32)
        piece = par[:, at].astype(F32) * keep
        top, low = piece[:rp], piece[rp:]
        packed.append(low_high(top, turned(low)))
        packed.append(low_high(turned(top), low))
        piece = piece.astype(BF16)
        for j in range(nj):
            slots[j, 2 * rt + m * rt : 2 * rt + (m + 1) * rt, :] = piece
    per_kid = nj // kids
    for j in range(nj):
        k, m = divmod(j, per_kid)
        at = slice(m * LANES, (m + 1) * LANES)
        keep = mask_kid_par[k, block_par, m * LANES // BLK].astype(F32)
        piece = kid_par[k, :, at].astype(F32) * keep
        slots[j, 0 : 2 * rp, :] = jnp.concatenate([piece, packed[j]], axis=0).astype(BF16)
        keep = mask_kid_top[k, block_top, m * LANES // BLK].astype(F32)
        slots[j, rt : 2 * rt, :] = (kid_top[k, :, at].astype(F32) * keep).astype(BF16)


def kid_par_columns(tall):
    ny, nj, rows, _ = tall.shape
    rp = rows // 2
    return tall[:, :, 0:rp, :].astype(F32).reshape(ny * nj * rp, LANES).astype(BF16)


def par_block(cols, m, rt):
    nj = cols.shape[0]
    return cols[:, 2 * rt + m * rt : 2 * rt + (m + 1) * rt, :].reshape(nj * rt, LANES)


def step_kernel(rt, cols, tall, send, step):
    nj = cols.shape[0]
    kid_par_j = kid_par_columns(tall)
    total = cols[:, rt : 2 * rt, :].astype(F32).reshape(nj * rt, LANES)
    for m in range(kid_par_j.shape[0] // LANES):
        total = total + dot(par_block(cols, m, rt), kid_par_j[m * LANES : (m + 1) * LANES])
    total = total.reshape(nj, rt, LANES)
    step[...] = total
    rounded = total.astype(BF16)
    for y in range(send.shape[0]):
        send[y] = rounded


def main_kernel(rt, rp, near, far, tall, step_j, cols, step, slots, part, db, xs):
    w1 = near.shape[-1]
    ny, nj = tall.shape[:2]
    x_me, c_me = lax.axis_index("x"), lax.axis_index("c")
    kid_par_j = kid_par_columns(tall)
    par_j = tall[:, :, rp : 2 * rp, :].astype(F32).reshape(ny * nj, 1, rp, LANES)
    par_j = jnp.concatenate([par_j, turned(par_j)], axis=1)
    par_j = par_j.reshape(ny * nj * 2 * rp, LANES).astype(BF16)
    both = jnp.concatenate([step_j[...].reshape(ny * nj * rt, LANES), par_j], axis=1)

    for b1, chunks in enumerate((near, far)):
        chunk_count = chunks.shape[0]
        s0 = chunks[:, 0:rt, :].reshape(chunk_count * rt, w1)
        s1 = chunks[:, rt : 2 * rt, :].reshape(chunk_count * rt, w1)
        d = chunks[:, 2 * rt : 2 * rt + rp, :].astype(F32).reshape(chunk_count * rp, w1)
        x = dot(s0, both[:w1]) + dot(s1, both[w1:])
        db_own = dot(d.astype(BF16), kid_par_j)
        for k in range(chunk_count):
            bc, b2, b4 = k // 4, (k // 2) % 2, k % 2
            chip = jnp.bitwise_xor(x_me, b1 + 2 * b2 + 4 * b4)
            at = 2 * chip + jnp.bitwise_xor(c_me, bc)
            piece = x[k * rt : (k + 1) * rt]
            xs[at] = piece.astype(BF16)
            part[at, 0:rt, :] = piece[:, :LANES].astype(BF16)
            c = piece[:, LANES:]
            part[at, rt : rt + rp, :] = low_high(c[:rp], turned(c[rp:])).astype(BF16)
            db[at] = db_own[k * rp : (k + 1) * rp]

    x = xs[...].reshape(nj * rt, 2 * LANES)
    for y in range(ny):
        partial = dot_t(par_block(cols, y, rt), x)
        rows = partial.shape[0]
        slots[y, 0:rows, :] = partial[:, :LANES].astype(BF16)
        q = partial[:, LANES:]
        q = low_high(q[: rows // 2], turned(q[rows // 2 :]))
        slots[y, rows : rows + rows // 2, :] = q.astype(BF16)
    kt = x[:, :LANES].astype(F32)
    var = jnp.sum(step[...].reshape(nj * rt, LANES) * kt, axis=0, keepdims=True)
    kid_par_tile = cols[:, 0:rp, :].astype(F32)
    var = var + jnp.sum((kid_par_tile * db[...]).reshape(nj * rp, LANES), axis=0, keepdims=True)
    var_rows = jnp.concatenate(split3(var) + [jnp.zeros((5, LANES), F32)], axis=0).astype(BF16)
    for y in range(ny):
        slots[y, rows + rows // 2 : rows + rows // 2 + 8, :] = var_rows


def sum_kernel(rt, rp, received, db, part, out):
    ny = received.shape[0]
    nj = out.shape[0]
    rows = nj * rp
    total = received[0].astype(F32)
    for y in range(1, ny):
        total = total + received[y].astype(F32)
    q = total[rows : rows + rows // 2]
    q = jnp.concatenate([q, turned(q)], axis=0)
    first = rows + rows // 2
    var = total[first : first + 1] + total[first + 1 : first + 2] + total[first + 2 : first + 3]
    var_rows = []
    for top in split3(var):
        var_rows += [turned(top), top]
    var_rows = jnp.concatenate(var_rows + [jnp.zeros((2, LANES), F32)], axis=0)
    for j in range(nj):
        at = slice(j * rp, (j + 1) * rp)
        out[j, 0 : rt + rp, :] = part[j]
        kp = total[at] + db[j]
        out[j, rt + rp : rt + 3 * rp, :] = jnp.concatenate(
            [kp, low_high(q[at], var_rows)], axis=0
        ).astype(BF16)


def final_kernel(rt, rp, got, dinv, dvar, cross_par, sigma_par, kid_top, kid_par, variance):
    nj = got.shape[0]
    kids = dvar.shape[0]
    per_kid = nj // kids
    for j in range(nj):
        k, m = divmod(j, per_kid)
        at = slice(m * LANES, (m + 1) * LANES)
        kid_top[k, :, at] = got[j, 0:rt, :]
        kid_par[k, :, at] = got[j, rt + rp : rt + 2 * rp, :]
        v = got[j, rt + 2 * rp : rt + 3 * rp, :].astype(F32)
        low = v[0:1] + v[2:3] + v[4:5]
        high = v[1:2] + v[3:4] + v[5:6]
        variance[k : k + 1, at] = dvar[k : k + 1, at] + low_high(turned(low), high)
    for m in range(nj // 2):
        at = slice(m * LANES, (m + 1) * LANES)
        a = got[2 * m, rt : rt + rp, :].astype(F32)
        b = got[2 * m + 1, rt : rt + rp, :].astype(F32)
        cross_par[:, at] = jnp.concatenate(
            [low_high(a, turned(b)), low_high(turned(a), b)], axis=0
        ).astype(BF16)
        a = got[2 * m, rt + 2 * rp : rt + 3 * rp, :].astype(F32)
        b = got[2 * m + 1, rt + 2 * rp : rt + 3 * rp, :].astype(F32)
        sigma_par[:, at] = (dinv[:, at] + low_high(a, turned(b))).astype(BF16)


def device_part(
    sigma_top,
    panel_par,
    dinv_par,
    panel_kid_top,
    panel_kid_par,
    dvar_kid,
    mask_par,
    mask_kid_top,
    mask_kid_par,
):
    rt, wt = sigma_top.shape
    rp, w1 = dinv_par.shape
    kids, _, w2 = panel_kid_top.shape
    ny = lax.axis_size("y")
    nx = lax.axis_size("x")
    nj = lax.axis_size(XC)
    assert kids * w2 == nj * LANES and w1 == nj * HALF and wt == 2 * w1
    assert nx == 8 and rt == 2 * rp and nj * rp == LANES and ny * LANES == w1

    slots, own = call(
        pack_kernel,
        [((nj, 2 * rt + w1 // LANES * rt, LANES), BF16), ((2 * rt + rp, w1), BF16)],
        (
            sigma_top,
            panel_par,
            dinv_par,
            panel_kid_top,
            panel_kid_par,
            mask_par,
            mask_kid_top,
            mask_kid_par,
        ),
        [VMEM] * 5 + [SMEM] * 3,
    )
    cols = exchanged(slots, XC)
    two = jnp.stack([own, swapped(own, "x", 4)])
    tall = sent_to_all(cols[:, : 2 * rp], "y")
    four = jnp.concatenate([two, swapped(two, "x", 2)])
    near = jnp.concatenate([four, swapped(four, "c", 1)])
    far = swapped(near, "x", 1)

    def sized(kernel):
        return lambda *refs: kernel(rt, rp, *refs)

    send, step = call(
        lambda *refs: step_kernel(rt, *refs),
        [((ny, nj, rt, LANES), BF16), ((nj, rt, LANES), F32)],
        (cols, tall),
    )
    step_j = exchanged(send, "y")
    rows4 = nj * rp + nj * rp // 2 + 8
    slots4, part, db = call(
        sized(main_kernel),
        [((ny, rows4, LANES), BF16), ((nj, rt + rp, LANES), BF16), ((nj, rp, LANES), F32)],
        (near, far, tall, step_j, cols, step),
        scratch=[pltpu.VMEM((nj, rt, 2 * LANES), BF16)],
    )
    received = exchanged(slots4, "y")
    (out,) = call(
        sized(sum_kernel), [((nj, rt + 3 * rp, LANES), BF16)], (received, db, part)
    )
    got = exchanged(out, XC)
    return call(
        sized(final_kernel),
        [
            ((rt, w1), BF16),
            ((rp, w1), BF16),
            ((kids, rt, w2), BF16),
            ((kids, rp, w2), BF16),
            ((kids, w2), F32),
        ],
        (got, dinv_par, dvar_kid),
    )


def solution(mesh):
    finer = Mesh(mesh.devices.reshape(mesh.shape["parts"], 8, 8, 2), PARTS_ROW)
    return jax.shard_map(
        device_part,
        mesh=finer,
        in_specs=(
            P(PARTS_ROW, None),
            P(PARTS_ROW, None),
            P(PARTS_ROW, None),
            P("parts", ROW, None),
            P("parts", ROW, None),
            P("parts", None),
            P("parts", None),
            P("parts", None, None),
            P("parts", None, None),
        ),
        out_specs=(
            P(PARTS_ROW, None),
            P(PARTS_ROW, None),
            P("parts", ROW, None),
            P("parts", ROW, None),
            P("parts", None),
        ),
        check_vma=False,
    )
```

```python
import jax
import jax.numpy as jnp
from jax import lax
from jax.experimental import pallas as pl
from jax.experimental.pallas import tpu as pltpu
from jax.sharding import Mesh
from jax.sharding import PartitionSpec as P

BLK = 256
LANES = 128
HALF = LANES // 2
ROW = ("y", "x", "c")
PARTS_ROW = ("parts", "y", "x", "c")
XC = ("x", "c")
F32 = jnp.float32
BF16 = jnp.bfloat16
VMEM = pl.BlockSpec(memory_space=pltpu.VMEM)
SMEM = pl.BlockSpec(memory_space=pltpu.SMEM)


def exchanged(x, axes):
    return lax.all_to_all(x, axes, split_axis=0, concat_axis=0, tiled=True)


def sent_to_all(x, axes):
    return exchanged(jnp.broadcast_to(x, (lax.axis_size(axes), *x.shape)), axes)


def swapped(x, axis, bit):
    return lax.ppermute(x, axis, [(i, i ^ bit) for i in range(lax.axis_size(axis))])


def dot(a, b):
    return jnp.dot(a, b, preferred_element_type=F32)


def dot_t(a, b):
    return lax.dot_general(a, b, (((0,), (0,)), ((), ())), preferred_element_type=F32)


def turned(x):
    return pltpu.roll(x, HALF, x.ndim - 1)


def low_high(low, high):
    lane = lax.broadcasted_iota(jnp.int32, low.shape, low.ndim - 1)
    return jnp.where(lane < HALF, low, high)


def split3(v):
    parts = []
    for _ in range(3):
        top = v.astype(BF16).astype(F32)
        parts.append(top)
        v = v - top
    return parts


def call(kernel, outs, args, specs=None, scratch=()):
    return pl.pallas_call(
        kernel,
        out_shape=tuple(jax.ShapeDtypeStruct(s, d) for s, d in outs),
        in_specs=specs or [VMEM] * len(args),
        out_specs=tuple(VMEM for _ in outs),
        scratch_shapes=scratch,
        compiler_params=pltpu.CompilerParams(vmem_limit_bytes=48 * 2**20),
    )(*args)


def pack_kernel(*refs):
    sources, (slots, own), scratch, done = refs[:8], refs[8:10], refs[10:18], refs[18]
    pairs = enumerate(zip(sources, scratch))
    copies = [pltpu.make_async_copy(a, b, done.at[i]) for i, (a, b) in pairs]
    for copy in copies:
        copy.start()
    for copy in copies:
        copy.wait()
    sigma, par, dinv, kid_top, kid_par, mask_par, mask_kid_top, mask_kid_par = scratch
    rt, w1 = par.shape
    rp = dinv.shape[0]
    kids = kid_top.shape[0]
    nj = slots.shape[0]
    position = lax.axis_index(ROW)
    block_top = lax.div(position * rt, BLK)
    block_par = lax.div(position * rp, BLK)
    own[rt : 2 * rt, :] = sigma[:, 0:w1]
    own[2 * rt : 3 * rt, :] = sigma[:, w1 : 2 * w1]
    own[3 * rt : 3 * rt + rp, :] = dinv[...].astype(BF16)

    def top_row(mask):
        lane = lax.broadcasted_iota(jnp.int32, mask.shape, 1)
        return jnp.sum(jnp.where(lane == block_top, mask, 0).astype(F32), axis=1, keepdims=True)

    keep = top_row(mask_par[...])
    packed = []
    for m in range(w1 // LANES):
        at = slice(m * LANES, (m + 1) * LANES)
        block = m * LANES // BLK
        piece = par[:, at].astype(F32) * keep[block : block + 1]
        top, low = piece[:rp], piece[rp:]
        packed.append(low_high(top, turned(low)))
        packed.append(low_high(turned(top), low))
        own[0:rt, at] = piece.astype(BF16)
    per_kid = nj // kids
    for k in range(kids):
        keep_top = top_row(mask_kid_top[k])
        keep_par = mask_kid_par[k, pl.ds(block_par, 1), :].astype(F32)
        for m in range(per_kid):
            j = k * per_kid + m
            at = slice(m * LANES, (m + 1) * LANES)
            block = m * LANES // BLK
            piece = kid_par[k, :, at].astype(F32) * keep_par[:, block : block + 1]
            slots[j, 0 : 2 * rp, :] = jnp.concatenate([piece, packed[j]], axis=0).astype(BF16)
            piece = kid_top[k, :, at].astype(F32) * keep_top[block : block + 1]
            slots[j, 2 * rp : 2 * rp + rt, :] = piece.astype(BF16)


def kid_par_columns(tall):
    ny, nj, rows, _ = tall.shape
    rp = rows // 2
    return tall[:, :, 0:rp, :].astype(F32).reshape(ny * nj * rp, LANES).astype(BF16)


def chunk_place(x_me, c_me, bits):
    b1, b2, b4, bc = bits
    return 2 * jnp.bitwise_xor(x_me, b1 + 2 * b2 + 4 * b4) + jnp.bitwise_xor(c_me, bc)


def step_kernel(rt, rp, cols, tall, par_own, par_other, send, step):
    x_me, c_me = lax.axis_index("x"), lax.axis_index("c")
    kid_par_j = kid_par_columns(tall)
    for bc, par in enumerate((par_own, par_other)):
        count, _, w1 = par.shape
        product = dot(par[...].reshape(count * rt, w1), kid_par_j)
        for k in range(count):
            at = chunk_place(x_me, c_me, (k // 4, (k // 2) % 2, k % 2, bc))
            total = cols[at, 2 * rp : 2 * rp + rt, :].astype(F32) + product[k * rt : (k + 1) * rt]
            step[at] = total
            rounded = total.astype(BF16)
            for y in range(send.shape[0]):
                send[y, at] = rounded


def main_kernel(
    rt, rp, near, far, par_own, par_other, tall, step_j, cols, step, slots, part, db
):
    w1 = near.shape[-1]
    ny, nj = tall.shape[:2]
    x_me, c_me = lax.axis_index("x"), lax.axis_index("c")
    kid_par_j = kid_par_columns(tall)
    par_j = tall[:, :, rp : 2 * rp, :].astype(F32).reshape(ny * nj, 1, rp, LANES)
    par_j = jnp.concatenate([par_j, turned(par_j)], axis=1)
    par_j = par_j.reshape(ny * nj * 2 * rp, LANES).astype(BF16)
    both = jnp.concatenate([step_j[...].reshape(ny * nj * rt, LANES), par_j], axis=1)

    var = jnp.zeros((1, LANES), F32)
    xs, ps = [], []
    for b1, chunks in enumerate((near, far)):
        count = chunks.shape[0]
        s0 = chunks[:, 0:rt, :].reshape(count * rt, w1)
        s1 = chunks[:, rt : 2 * rt, :].reshape(count * rt, w1)
        d = chunks[:, 2 * rt : 2 * rt + rp, :].astype(F32).reshape(count * rp, w1)
        x = dot(s0, both[:w1]) + dot(s1, both[w1:])
        db_own = dot(d.astype(BF16), kid_par_j)
        for k in range(count):
            at = chunk_place(x_me, c_me, (b1, (k // 2) % 2, k % 2, k // 4))
            piece = x[k * rt : (k + 1) * rt]
            kt = piece[:, :LANES].astype(BF16)
            part[at, 0:rt, :] = kt
            c = piece[:, LANES:]
            part[at, rt : rt + rp, :] = low_high(c[:rp], turned(c[rp:])).astype(BF16)
            db_k = db_own[k * rp : (k + 1) * rp]
            db[at] = db_k
            var = var + jnp.sum(step[at] * kt.astype(F32), axis=0, keepdims=True)
            var = var + jnp.sum(cols[at, 0:rp, :].astype(F32) * db_k, axis=0, keepdims=True)
        xs.append(x.astype(BF16))
        for par in (par_own, par_other):
            ps.append(par[4 * b1 : 4 * b1 + 4].reshape(4 * rt, w1))

    x = jnp.concatenate(xs, axis=0)
    p = jnp.concatenate(ps, axis=0)
    for y in range(ny):
        partial = dot_t(p[:, y * LANES : (y + 1) * LANES], x)
        rows = partial.shape[0]
        slots[y, 0:rows, :] = partial[:, :LANES].astype(BF16)
        q = partial[:, LANES:]
        q = low_high(q[: rows // 2], turned(q[rows // 2 :]))
        slots[y, rows : rows + rows // 2, :] = q.astype(BF16)
    var_rows = jnp.concatenate(split3(var) + [jnp.zeros((5, LANES), F32)], axis=0).astype(BF16)
    for y in range(ny):
        slots[y, rows + rows // 2 : rows + rows // 2 + 8, :] = var_rows


def sum_kernel(rt, rp, received, db, part, out):
    ny = received.shape[0]
    nj = out.shape[0]
    rows = nj * rp
    total = received[0].astype(F32)
    for y in range(1, ny):
        total = total + received[y].astype(F32)
    q = total[rows : rows + rows // 2]
    q = jnp.concatenate([q, turned(q)], axis=0)
    first = rows + rows // 2
    var = total[first : first + 1] + total[first + 1 : first + 2] + total[first + 2 : first + 3]
    var_rows = []
    for top in split3(var):
        var_rows += [turned(top), top]
    var_rows = jnp.concatenate(var_rows + [jnp.zeros((2, LANES), F32)], axis=0)
    for j in range(nj):
        at = slice(j * rp, (j + 1) * rp)
        out[j, 0 : rt + rp, :] = part[j]
        kp = total[at] + db[j]
        out[j, rt + rp : rt + 3 * rp, :] = jnp.concatenate(
            [kp, low_high(q[at], var_rows)], axis=0
        ).astype(BF16)


def final_kernel(rt, rp, got, dinv, dvar, cross_par, sigma_par, kid_top, kid_par, variance):
    nj = got.shape[0]
    kids = dvar.shape[0]
    per_kid = nj // kids
    for j in range(nj):
        k, m = divmod(j, per_kid)
        at = slice(m * LANES, (m + 1) * LANES)
        kid_top[k, :, at] = got[j, 0:rt, :]
        kid_par[k, :, at] = got[j, rt + rp : rt + 2 * rp, :]
        v = got[j, rt + 2 * rp : rt + 3 * rp, :].astype(F32)
        low = v[0:1] + v[2:3] + v[4:5]
        high = v[1:2] + v[3:4] + v[5:6]
        variance[k : k + 1, at] = dvar[k : k + 1, at] + low_high(turned(low), high)
    for m in range(nj // 2):
        at = slice(m * LANES, (m + 1) * LANES)
        a = got[2 * m, rt : rt + rp, :].astype(F32)
        b = got[2 * m + 1, rt : rt + rp, :].astype(F32)
        cross_par[:, at] = jnp.concatenate(
            [low_high(a, turned(b)), low_high(turned(a), b)], axis=0
        ).astype(BF16)
        a = got[2 * m, rt + 2 * rp : rt + 3 * rp, :].astype(F32)
        b = got[2 * m + 1, rt + 2 * rp : rt + 3 * rp, :].astype(F32)
        sigma_par[:, at] = (dinv[:, at] + low_high(a, turned(b))).astype(BF16)


def device_part(
    sigma_top,
    panel_par,
    dinv_par,
    panel_kid_top,
    panel_kid_par,
    dvar_kid,
    mask_par,
    mask_kid_top,
    mask_kid_par,
):
    rt, wt = sigma_top.shape
    rp, w1 = dinv_par.shape
    kids, _, w2 = panel_kid_top.shape
    ny = lax.axis_size("y")
    nx = lax.axis_size("x")
    nj = lax.axis_size(XC)
    assert kids * w2 == nj * LANES and w1 == nj * HALF and wt == 2 * w1
    assert nx == 8 and rt == 2 * rp and nj * rp == LANES and ny * LANES == w1

    arrays = (
        sigma_top,
        panel_par,
        dinv_par,
        panel_kid_top,
        panel_kid_par,
        mask_par.T,
        mask_kid_top.transpose(0, 2, 1),
        mask_kid_par,
    )
    slots, own = call(
        pack_kernel,
        [((nj, 2 * rp + rt, LANES), BF16), ((3 * rt + rp, w1), BF16)],
        tuple(pltpu.with_memory_space_constraint(a, pltpu.HBM) for a in arrays),
        [pl.BlockSpec(memory_space=pltpu.HBM)] * len(arrays),
        [pltpu.VMEM(a.shape, a.dtype) for a in arrays]
        + [pltpu.SemaphoreType.DMA((len(arrays),))],
    )
    own_4 = swapped(own, "x", 4)
    cols = exchanged(slots, XC)
    two = jnp.stack([own, own_4])
    tall = sent_to_all(cols[:, : 2 * rp], "y")
    two_2 = swapped(two, "x", 2)
    par_four = jnp.concatenate([two[:, :rt], two_2[:, :rt]])
    four = jnp.concatenate([two[:, rt:], two_2[:, rt:]])
    par_own = jnp.concatenate([par_four, swapped(par_four, "x", 1)])
    par_other = swapped(par_own, "c", 1)
    near = jnp.concatenate([four, swapped(four, "c", 1)])
    far = swapped(near, "x", 1)

    def sized(kernel):
        return lambda *refs: kernel(rt, rp, *refs)

    send, step = call(
        sized(step_kernel),
        [((ny, nj, rt, LANES), BF16), ((nj, rt, LANES), F32)],
        (cols, tall, par_own, par_other),
    )
    step_j = exchanged(send, "y")
    rows4 = nj * rp + nj * rp // 2 + 8
    slots4, part, db = call(
        sized(main_kernel),
        [((ny, rows4, LANES), BF16), ((nj, rt + rp, LANES), BF16), ((nj, rp, LANES), F32)],
        (near, far, par_own, par_other, tall, step_j, cols, step),
    )
    received = exchanged(slots4, "y")
    (out,) = call(
        sized(sum_kernel), [((nj, rt + 3 * rp, LANES), BF16)], (received, db, part)
    )
    got = exchanged(out, XC)
    return call(
        sized(final_kernel),
        [
            ((rt, w1), BF16),
            ((rp, w1), BF16),
            ((kids, rt, w2), BF16),
            ((kids, rp, w2), BF16),
            ((kids, w2), F32),
        ],
        (got, dinv_par, dvar_kid),
    )


def solution(mesh):
    finer = Mesh(mesh.devices.reshape(mesh.shape["parts"], 8, 8, 2), PARTS_ROW)
    return jax.shard_map(
        device_part,
        mesh=finer,
        in_specs=(
            P(PARTS_ROW, None),
            P(PARTS_ROW, None),
            P(PARTS_ROW, None),
            P("parts", ROW, None),
            P("parts", ROW, None),
            P("parts", None),
            P("parts", None),
            P("parts", None, None),
            P("parts", None, None),
        ),
        out_specs=(
            P(PARTS_ROW, None),
            P(PARTS_ROW, None),
            P("parts", ROW, None),
            P("parts", ROW, None),
            P("parts", None),
        ),
        check_vma=False,
    )
```

```python
import jax
import jax.numpy as jnp
from jax import lax
from jax.experimental import pallas as pl
from jax.experimental.pallas import tpu as pltpu
from jax.sharding import Mesh
from jax.sharding import PartitionSpec as P

BLK = 256
LANES = 128
HALF = LANES // 2
ROW = ("y", "x", "c")
PARTS_ROW = ("parts", "y", "x", "c")
XC = ("x", "c")
F32 = jnp.float32
BF16 = jnp.bfloat16
VMEM = pl.BlockSpec(memory_space=pltpu.VMEM)
SMEM = pl.BlockSpec(memory_space=pltpu.SMEM)


def exchanged(x, axes):
    return lax.all_to_all(x, axes, split_axis=0, concat_axis=0, tiled=True)


def sent_to_all(x, axes):
    return exchanged(jnp.broadcast_to(x, (lax.axis_size(axes), *x.shape)), axes)


def swapped(x, axis, bit):
    return lax.ppermute(x, axis, [(i, i ^ bit) for i in range(lax.axis_size(axis))])


def dot(a, b):
    return jnp.dot(a, b, preferred_element_type=F32)


def dot_t(a, b):
    return lax.dot_general(a, b, (((0,), (0,)), ((), ())), preferred_element_type=F32)


def turned(x):
    return pltpu.roll(x, HALF, x.ndim - 1)


def low_high(low, high):
    lane = lax.broadcasted_iota(jnp.int32, low.shape, low.ndim - 1)
    return jnp.where(lane < HALF, low, high)


def split3(v):
    parts = []
    for _ in range(3):
        top = v.astype(BF16).astype(F32)
        parts.append(top)
        v = v - top
    return parts


def call(kernel, outs, args, specs=None, scratch=()):
    return pl.pallas_call(
        kernel,
        out_shape=tuple(jax.ShapeDtypeStruct(s, d) for s, d in outs),
        in_specs=specs or [VMEM] * len(args),
        out_specs=tuple(VMEM for _ in outs),
        scratch_shapes=scratch,
        compiler_params=pltpu.CompilerParams(vmem_limit_bytes=48 * 2**20),
    )(*args)


def fetched(sources, scratch, done):
    pairs = enumerate(zip(sources, scratch))
    copies = [pltpu.make_async_copy(a, b, done.at[i]) for i, (a, b) in pairs]
    for copy in copies:
        copy.start()
    for copy in copies:
        copy.wait()


def lane_of(mask, at):
    lane = lax.broadcasted_iota(jnp.int32, mask.shape, 1)
    return jnp.sum(jnp.where(lane == at, mask, 0).astype(F32), axis=1, keepdims=True)


def slots_kernel(*refs):
    sources, slots, scratch, done = refs[:6], refs[6], refs[7:13], refs[13]
    fetched(sources, scratch, done)
    par, kid_top, kid_par, mask_par, mask_kid_top, mask_kid_par = scratch
    rt, w1 = par.shape
    kids, rp = kid_par.shape[:2]
    nj = slots.shape[0]
    position = lax.axis_index(ROW)
    block_top = lax.div(position * rt, BLK)
    block_par = lax.div(position * rp, BLK)
    keep = lane_of(mask_par[...], block_top)
    packed = []
    for m in range(w1 // LANES):
        at = slice(m * LANES, (m + 1) * LANES)
        block = m * LANES // BLK
        piece = par[:, at].astype(F32) * keep[block : block + 1]
        top, low = piece[:rp], piece[rp:]
        packed.append(low_high(top, turned(low)))
        packed.append(low_high(turned(top), low))
    per_kid = nj // kids
    for k in range(kids):
        keep_top = lane_of(mask_kid_top[k], block_top)
        keep_par = mask_kid_par[k, pl.ds(block_par, 1), :].astype(F32)
        for m in range(per_kid):
            j = k * per_kid + m
            at = slice(m * LANES, (m + 1) * LANES)
            block = m * LANES // BLK
            piece = kid_par[k, :, at].astype(F32) * keep_par[:, block : block + 1]
            slots[j, 0 : 2 * rp, :] = jnp.concatenate([piece, packed[j]], axis=0).astype(BF16)
            piece = kid_top[k, :, at].astype(F32) * keep_top[block : block + 1]
            slots[j, 2 * rp : 2 * rp + rt, :] = piece.astype(BF16)


def masked_kernel(par_hbm, mask_hbm, masked, par, mask_par, done):
    fetched((par_hbm, mask_hbm), (par, mask_par), done)
    rt, w1 = par.shape
    keep = lane_of(mask_par[...], lax.div(lax.axis_index(ROW) * rt, BLK))
    for b in range(w1 // BLK):
        at = slice(b * BLK, (b + 1) * BLK)
        masked[:, at] = (par[:, at].astype(F32) * keep[b : b + 1]).astype(BF16)


def rows_kernel(sigma_hbm, dinv_hbm, rows, sigma, dinv, done):
    fetched((sigma_hbm, dinv_hbm), (sigma, dinv), done)
    rt = sigma.shape[0]
    rp, w1 = dinv.shape
    rows[0:rt, :] = sigma[:, 0:w1]
    rows[rt : 2 * rt, :] = sigma[:, w1 : 2 * w1]
    rows[2 * rt : 2 * rt + rp, :] = dinv[...].astype(BF16)


def copy_kernel(source_hbm, result, scratch, done):
    fetched((source_hbm,), (scratch,), done)
    result[...] = scratch[...]


def kid_par_columns(tall):
    ny, nj, rows, _ = tall.shape
    rp = rows // 2
    return tall[:, :, 0:rp, :].astype(F32).reshape(ny * nj * rp, LANES).astype(BF16)


def chunk_place(x_me, c_me, bits):
    b1, b2, b4, bc = bits
    return 2 * jnp.bitwise_xor(x_me, b1 + 2 * b2 + 4 * b4) + jnp.bitwise_xor(c_me, bc)


def step_kernel(rt, rp, cols, tall, par_own, par_other, send, step):
    x_me, c_me = lax.axis_index("x"), lax.axis_index("c")
    kid_par_j = kid_par_columns(tall)
    for bc, par in enumerate((par_own, par_other)):
        count, _, w1 = par.shape
        product = dot(par[...].reshape(count * rt, w1), kid_par_j)
        for k in range(count):
            at = chunk_place(x_me, c_me, (k // 4, (k // 2) % 2, k % 2, bc))
            total = cols[at, 2 * rp : 2 * rp + rt, :].astype(F32) + product[k * rt : (k + 1) * rt]
            step[at] = total
            rounded = total.astype(BF16)
            for y in range(send.shape[0]):
                send[y, at] = rounded


def main_kernel(
    rt, rp, near, far, par_own, par_other, tall, step_j, cols, step, slots, part, db
):
    w1 = near.shape[-1]
    ny, nj = tall.shape[:2]
    x_me, c_me = lax.axis_index("x"), lax.axis_index("c")
    kid_par_j = kid_par_columns(tall)
    par_j = tall[:, :, rp : 2 * rp, :].astype(F32).reshape(ny * nj, 1, rp, LANES)
    par_j = jnp.concatenate([par_j, turned(par_j)], axis=1)
    par_j = par_j.reshape(ny * nj * 2 * rp, LANES).astype(BF16)
    both = jnp.concatenate([step_j[...].reshape(ny * nj * rt, LANES), par_j], axis=1)

    var = jnp.zeros((1, LANES), F32)
    xs = []
    for bc, chunks in enumerate((near, far)):
        count = chunks.shape[0]
        s0 = chunks[:, 0:rt, :].reshape(count * rt, w1)
        s1 = chunks[:, rt : 2 * rt, :].reshape(count * rt, w1)
        d = chunks[:, 2 * rt : 2 * rt + rp, :].astype(F32).reshape(count * rp, w1)
        x = dot(s0, both[:w1]) + dot(s1, both[w1:])
        db_own = dot(d.astype(BF16), kid_par_j)
        for k in range(count):
            at = chunk_place(x_me, c_me, (k // 4, (k // 2) % 2, k % 2, bc))
            piece = x[k * rt : (k + 1) * rt]
            kt = piece[:, :LANES].astype(BF16)
            part[at, 0:rt, :] = kt
            c = piece[:, LANES:]
            part[at, rt : rt + rp, :] = low_high(c[:rp], turned(c[rp:])).astype(BF16)
            db_k = db_own[k * rp : (k + 1) * rp]
            db[at] = db_k
            var = var + jnp.sum(step[at] * kt.astype(F32), axis=0, keepdims=True)
            var = var + jnp.sum(cols[at, 0:rp, :].astype(F32) * db_k, axis=0, keepdims=True)
        xs.append(x.astype(BF16))

    x = jnp.concatenate(xs, axis=0)
    p = jnp.concatenate([p[...].reshape(nj // 2 * rt, w1) for p in (par_own, par_other)], axis=0)
    for y in range(ny):
        partial = dot_t(p[:, y * LANES : (y + 1) * LANES], x)
        rows = partial.shape[0]
        slots[y, 0:rows, :] = partial[:, :LANES].astype(BF16)
        q = partial[:, LANES:]
        q = low_high(q[: rows // 2], turned(q[rows // 2 :]))
        slots[y, rows : rows + rows // 2, :] = q.astype(BF16)
    var_rows = jnp.concatenate(split3(var) + [jnp.zeros((5, LANES), F32)], axis=0).astype(BF16)
    for y in range(ny):
        slots[y, rows + rows // 2 : rows + rows // 2 + 8, :] = var_rows


def sum_kernel(rt, rp, received, db, part, out):
    ny = received.shape[0]
    nj = out.shape[0]
    rows = nj * rp
    total = received[0].astype(F32)
    for y in range(1, ny):
        total = total + received[y].astype(F32)
    q = total[rows : rows + rows // 2]
    q = jnp.concatenate([q, turned(q)], axis=0)
    first = rows + rows // 2
    var = total[first : first + 1] + total[first + 1 : first + 2] + total[first + 2 : first + 3]
    var_rows = []
    for top in split3(var):
        var_rows += [turned(top), top]
    var_rows = jnp.concatenate(var_rows + [jnp.zeros((2, LANES), F32)], axis=0)
    for j in range(nj):
        at = slice(j * rp, (j + 1) * rp)
        out[j, 0 : rt + rp, :] = part[j]
        kp = total[at] + db[j]
        out[j, rt + rp : rt + 3 * rp, :] = jnp.concatenate(
            [kp, low_high(q[at], var_rows)], axis=0
        ).astype(BF16)


def final_kernel(rt, rp, got, dinv, dvar, cross_par, sigma_par, kid_top, kid_par, variance):
    nj = got.shape[0]
    kids = dvar.shape[0]
    per_kid = nj // kids
    for j in range(nj):
        k, m = divmod(j, per_kid)
        at = slice(m * LANES, (m + 1) * LANES)
        kid_top[k, :, at] = got[j, 0:rt, :]
        kid_par[k, :, at] = got[j, rt + rp : rt + 2 * rp, :]
        v = got[j, rt + 2 * rp : rt + 3 * rp, :].astype(F32)
        low = v[0:1] + v[2:3] + v[4:5]
        high = v[1:2] + v[3:4] + v[5:6]
        variance[k : k + 1, at] = dvar[k : k + 1, at] + low_high(turned(low), high)
    for m in range(nj // 2):
        at = slice(m * LANES, (m + 1) * LANES)
        a = got[2 * m, rt : rt + rp, :].astype(F32)
        b = got[2 * m + 1, rt : rt + rp, :].astype(F32)
        cross_par[:, at] = jnp.concatenate(
            [low_high(a, turned(b)), low_high(turned(a), b)], axis=0
        ).astype(BF16)
        a = got[2 * m, rt + 2 * rp : rt + 3 * rp, :].astype(F32)
        b = got[2 * m + 1, rt + 2 * rp : rt + 3 * rp, :].astype(F32)
        sigma_par[:, at] = (dinv[:, at] + low_high(a, turned(b))).astype(BF16)


def device_part(
    sigma_top,
    panel_par,
    dinv_par,
    panel_kid_top,
    panel_kid_par,
    dvar_kid,
    mask_par,
    mask_kid_top,
    mask_kid_par,
):
    rt, wt = sigma_top.shape
    rp, w1 = dinv_par.shape
    kids, _, w2 = panel_kid_top.shape
    ny = lax.axis_size("y")
    nx = lax.axis_size("x")
    nj = lax.axis_size(XC)
    assert kids * w2 == nj * LANES and w1 == nj * HALF and wt == 2 * w1
    assert nx == 8 and rt == 2 * rp and nj * rp == LANES and ny * LANES == w1

    def fetching(kernel, outs, arrays):
        return call(
            kernel,
            outs,
            tuple(pltpu.with_memory_space_constraint(a, pltpu.HBM) for a in arrays),
            [pl.BlockSpec(memory_space=pltpu.HBM)] * len(arrays),
            [pltpu.VMEM(a.shape, a.dtype) for a in arrays]
            + [pltpu.SemaphoreType.DMA((len(arrays),))],
        )

    masks = (mask_par.T, mask_kid_top.transpose(0, 2, 1), mask_kid_par)
    (slots,) = fetching(
        slots_kernel,
        [((nj, 2 * rp + rt, LANES), BF16)],
        (panel_par, panel_kid_top, panel_kid_par, *masks),
    )
    cols = exchanged(slots, XC)
    (par_rows,) = fetching(masked_kernel, [((rt, w1), BF16)], (panel_par, masks[0]))
    par_rows = jnp.stack([par_rows, swapped(par_rows, "x", 4)])
    (rows,) = fetching(rows_kernel, [((2 * rt + rp, w1), BF16)], (sigma_top, dinv_par))
    rows = jnp.stack([rows, swapped(rows, "x", 4)])
    (dvar_kid,) = fetching(copy_kernel, [(dvar_kid.shape, F32)], (dvar_kid,))
    tall = sent_to_all(cols[:, : 2 * rp], "y")
    par_rows = jnp.concatenate([par_rows, swapped(par_rows, "x", 2)])
    par_own = jnp.concatenate([par_rows, swapped(par_rows, "x", 1)])
    par_other = swapped(par_own, "c", 1)
    rows = jnp.concatenate([rows, swapped(rows, "x", 2)])
    near = jnp.concatenate([rows, swapped(rows, "x", 1)])
    far = swapped(near, "c", 1)

    def sized(kernel):
        return lambda *refs: kernel(rt, rp, *refs)

    send, step = call(
        sized(step_kernel),
        [((ny, nj, rt, LANES), BF16), ((nj, rt, LANES), F32)],
        (cols, tall, par_own, par_other),
    )
    step_j = exchanged(send, "y")
    rows4 = nj * rp + nj * rp // 2 + 8
    slots4, part, db = call(
        sized(main_kernel),
        [((ny, rows4, LANES), BF16), ((nj, rt + rp, LANES), BF16), ((nj, rp, LANES), F32)],
        (near, far, par_own, par_other, tall, step_j, cols, step),
    )
    received = exchanged(slots4, "y")
    (out,) = call(
        sized(sum_kernel), [((nj, rt + 3 * rp, LANES), BF16)], (received, db, part)
    )
    got = exchanged(out, XC)
    return call(
        sized(final_kernel),
        [
            ((rt, w1), BF16),
            ((rp, w1), BF16),
            ((kids, rt, w2), BF16),
            ((kids, rp, w2), BF16),
            ((kids, w2), F32),
        ],
        (got, dinv_par, dvar_kid),
    )


def solution(mesh):
    finer = Mesh(mesh.devices.reshape(mesh.shape["parts"], 8, 8, 2), PARTS_ROW)
    return jax.shard_map(
        device_part,
        mesh=finer,
        in_specs=(
            P(PARTS_ROW, None),
            P(PARTS_ROW, None),
            P(PARTS_ROW, None),
            P("parts", ROW, None),
            P("parts", ROW, None),
            P("parts", None),
            P("parts", None),
            P("parts", None, None),
            P("parts", None, None),
        ),
        out_specs=(
            P(PARTS_ROW, None),
            P(PARTS_ROW, None),
            P("parts", ROW, None),
            P("parts", ROW, None),
            P("parts", None),
        ),
        check_vma=False,
    )
```

```python
import jax
import jax.numpy as jnp
from jax import lax
from jax.experimental import pallas as pl
from jax.experimental.pallas import tpu as pltpu
from jax.sharding import Mesh
from jax.sharding import PartitionSpec as P

BLK = 256
LANES = 128
HALF = LANES // 2
ROW = ("y", "x", "c")
PARTS_ROW = ("parts", "y", "x", "c")
XC = ("x", "c")
F32 = jnp.float32
BF16 = jnp.bfloat16
VMEM = pl.BlockSpec(memory_space=pltpu.VMEM)
SMEM = pl.BlockSpec(memory_space=pltpu.SMEM)


def exchanged(x, axes):
    return lax.all_to_all(x, axes, split_axis=0, concat_axis=0, tiled=True)


def swapped(x, axis, bit):
    return lax.ppermute(x, axis, [(i, i ^ bit) for i in range(lax.axis_size(axis))])


def dot(a, b):
    return jnp.dot(a, b, preferred_element_type=F32)


def dot_t(a, b):
    return lax.dot_general(a, b, (((0,), (0,)), ((), ())), preferred_element_type=F32)


def turned(x):
    return pltpu.roll(x, HALF, x.ndim - 1)


def low_high(low, high):
    lane = lax.broadcasted_iota(jnp.int32, low.shape, low.ndim - 1)
    return jnp.where(lane < HALF, low, high)


def split3(v):
    parts = []
    for _ in range(3):
        top = v.astype(BF16).astype(F32)
        parts.append(top)
        v = v - top
    return parts


def call(kernel, outs, args, specs=None, scratch=()):
    return pl.pallas_call(
        kernel,
        out_shape=tuple(jax.ShapeDtypeStruct(s, d) for s, d in outs),
        in_specs=specs or [VMEM] * len(args),
        out_specs=tuple(VMEM for _ in outs),
        scratch_shapes=scratch,
        compiler_params=pltpu.CompilerParams(vmem_limit_bytes=48 * 2**20),
    )(*args)


def fetched(sources, scratch, done):
    pairs = enumerate(zip(sources, scratch))
    copies = [pltpu.make_async_copy(a, b, done.at[i]) for i, (a, b) in pairs]
    for copy in copies:
        copy.start()
    for copy in copies:
        copy.wait()


def lane_of(mask, at):
    lane = lax.broadcasted_iota(jnp.int32, mask.shape, 1)
    return jnp.sum(jnp.where(lane == at, mask, 0).astype(F32), axis=1, keepdims=True)


def slots_kernel(*refs):
    sources, slots, scratch, done = refs[:6], refs[6], refs[7:13], refs[13]
    fetched(sources, scratch, done)
    par, kid_top, kid_par, mask_par, mask_kid_top, mask_kid_par = scratch
    rt, w1 = par.shape
    kids, rp = kid_par.shape[:2]
    nj = slots.shape[0]
    position = lax.axis_index(ROW)
    block_top = lax.div(position * rt, BLK)
    block_par = lax.div(position * rp, BLK)
    keep = lane_of(mask_par[...], block_top)
    packed = []
    for m in range(w1 // LANES):
        at = slice(m * LANES, (m + 1) * LANES)
        block = m * LANES // BLK
        piece = par[:, at].astype(F32) * keep[block : block + 1]
        top, low = piece[:rp], piece[rp:]
        packed.append(low_high(top, turned(low)))
        packed.append(low_high(turned(top), low))
    per_kid = nj // kids
    for k in range(kids):
        keep_top = lane_of(mask_kid_top[k], block_top)
        keep_par = mask_kid_par[k, pl.ds(block_par, 1), :].astype(F32)
        for m in range(per_kid):
            j = k * per_kid + m
            at = slice(m * LANES, (m + 1) * LANES)
            block = m * LANES // BLK
            piece = kid_par[k, :, at].astype(F32) * keep_par[:, block : block + 1]
            slots[j, 0 : 2 * rp, :] = jnp.concatenate([piece, packed[j]], axis=0).astype(BF16)
            piece = kid_top[k, :, at].astype(F32) * keep_top[block : block + 1]
            slots[j, 2 * rp : 2 * rp + rt, :] = piece.astype(BF16)


def rows_kernel(*refs):
    sources, rows, scratch, done = refs[:4], refs[4], refs[5:9], refs[9]
    fetched(sources, scratch, done)
    sigma, par, dinv, mask_par = scratch
    rt, w1 = par.shape
    rp = dinv.shape[0]
    keep = lane_of(mask_par[...], lax.div(lax.axis_index(ROW) * rt, BLK))
    for b in range(w1 // BLK):
        at = slice(b * BLK, (b + 1) * BLK)
        rows[0:rt, at] = (par[:, at].astype(F32) * keep[b : b + 1]).astype(BF16)
    rows[rt : 2 * rt, :] = sigma[:, 0:w1]
    rows[2 * rt : 3 * rt, :] = sigma[:, w1 : 2 * w1]
    rows[3 * rt : 3 * rt + rp, :] = dinv[...].astype(BF16)


def copy_kernel(source_hbm, result, scratch, done):
    fetched((source_hbm,), (scratch,), done)
    result[...] = scratch[...]


def stack_kernel(own, other, par_rows, rows):
    rt = par_rows.shape[1]
    for i, source in enumerate((own, other)):
        par_rows[i] = source[0:rt, :]
        rows[i] = source[rt : rt + rows.shape[1], :]


def join_kernel(own, other, joined):
    count = own.shape[0]
    joined[0:count] = own[...]
    joined[count : 2 * count] = other[...]


def repeat_kernel(cols, send):
    rows = send.shape[2]
    for y in range(send.shape[0]):
        send[y] = cols[:, 0:rows, :]


def kid_par_columns(tall):
    ny, nj, rows, _ = tall.shape
    rp = rows // 2
    return tall[:, :, 0:rp, :].astype(F32).reshape(ny * nj * rp, LANES).astype(BF16)


def chunk_place(x_me, c_me, bits):
    b1, b2, b4, bc = bits
    return 2 * jnp.bitwise_xor(x_me, b1 + 2 * b2 + 4 * b4) + jnp.bitwise_xor(c_me, bc)


def step_kernel(rt, rp, cols, tall, par_own, par_other, send, step):
    x_me, c_me = lax.axis_index("x"), lax.axis_index("c")
    kid_par_j = kid_par_columns(tall)
    for bc, par in enumerate((par_own, par_other)):
        count, _, w1 = par.shape
        product = dot(par[...].reshape(count * rt, w1), kid_par_j)
        for k in range(count):
            at = chunk_place(x_me, c_me, (k // 4, (k // 2) % 2, k % 2, bc))
            total = cols[at, 2 * rp : 2 * rp + rt, :].astype(F32) + product[k * rt : (k + 1) * rt]
            step[at] = total
            rounded = total.astype(BF16)
            for y in range(send.shape[0]):
                send[y, at] = rounded


def main_kernel(
    rt, rp, near, far, par_own, par_other, tall, step_j, cols, step, slots, part, db
):
    w1 = near.shape[-1]
    ny, nj = tall.shape[:2]
    x_me, c_me = lax.axis_index("x"), lax.axis_index("c")
    kid_par_j = kid_par_columns(tall)
    par_j = tall[:, :, rp : 2 * rp, :].astype(F32).reshape(ny * nj, 1, rp, LANES)
    par_j = jnp.concatenate([par_j, turned(par_j)], axis=1)
    par_j = par_j.reshape(ny * nj * 2 * rp, LANES).astype(BF16)
    both = jnp.concatenate([step_j[...].reshape(ny * nj * rt, LANES), par_j], axis=1)

    var = jnp.zeros((1, LANES), F32)
    xs = []
    for bc, chunks in enumerate((near, far)):
        count = chunks.shape[0]
        s0 = chunks[:, 0:rt, :].reshape(count * rt, w1)
        s1 = chunks[:, rt : 2 * rt, :].reshape(count * rt, w1)
        d = chunks[:, 2 * rt : 2 * rt + rp, :].astype(F32).reshape(count * rp, w1)
        x = dot(s0, both[:w1]) + dot(s1, both[w1:])
        db_own = dot(d.astype(BF16), kid_par_j)
        for k in range(count):
            at = chunk_place(x_me, c_me, (k // 4, (k // 2) % 2, k % 2, bc))
            piece = x[k * rt : (k + 1) * rt]
            kt = piece[:, :LANES].astype(BF16)
            part[at, 0:rt, :] = kt
            c = piece[:, LANES:]
            part[at, rt : rt + rp, :] = low_high(c[:rp], turned(c[rp:])).astype(BF16)
            db_k = db_own[k * rp : (k + 1) * rp]
            db[at] = db_k
            var = var + jnp.sum(step[at] * kt.astype(F32), axis=0, keepdims=True)
            var = var + jnp.sum(cols[at, 0:rp, :].astype(F32) * db_k, axis=0, keepdims=True)
        xs.append(x.astype(BF16))

    x = jnp.concatenate(xs, axis=0)
    p = jnp.concatenate([p[...].reshape(nj // 2 * rt, w1) for p in (par_own, par_other)], axis=0)
    for y in range(ny):
        partial = dot_t(p[:, y * LANES : (y + 1) * LANES], x)
        rows = partial.shape[0]
        slots[y, 0:rows, :] = partial[:, :LANES].astype(BF16)
        q = partial[:, LANES:]
        q = low_high(q[: rows // 2], turned(q[rows // 2 :]))
        slots[y, rows : rows + rows // 2, :] = q.astype(BF16)
    var_rows = jnp.concatenate(split3(var) + [jnp.zeros((5, LANES), F32)], axis=0).astype(BF16)
    for y in range(ny):
        slots[y, rows + rows // 2 : rows + rows // 2 + 8, :] = var_rows


def sum_kernel(rt, rp, received, db, part, out):
    ny = received.shape[0]
    nj = out.shape[0]
    rows = nj * rp
    total = received[0].astype(F32)
    for y in range(1, ny):
        total = total + received[y].astype(F32)
    q = total[rows : rows + rows // 2]
    q = jnp.concatenate([q, turned(q)], axis=0)
    first = rows + rows // 2
    var = total[first : first + 1] + total[first + 1 : first + 2] + total[first + 2 : first + 3]
    var_rows = []
    for top in split3(var):
        var_rows += [turned(top), top]
    var_rows = jnp.concatenate(var_rows + [jnp.zeros((2, LANES), F32)], axis=0)
    for j in range(nj):
        at = slice(j * rp, (j + 1) * rp)
        out[j, 0 : rt + rp, :] = part[j]
        kp = total[at] + db[j]
        out[j, rt + rp : rt + 3 * rp, :] = jnp.concatenate(
            [kp, low_high(q[at], var_rows)], axis=0
        ).astype(BF16)


def final_kernel(rt, rp, got, dinv, dvar, cross_par, sigma_par, kid_top, kid_par, variance):
    nj = got.shape[0]
    kids = dvar.shape[0]
    per_kid = nj // kids
    for j in range(nj):
        k, m = divmod(j, per_kid)
        at = slice(m * LANES, (m + 1) * LANES)
        kid_top[k, :, at] = got[j, 0:rt, :]
        kid_par[k, :, at] = got[j, rt + rp : rt + 2 * rp, :]
        v = got[j, rt + 2 * rp : rt + 3 * rp, :].astype(F32)
        low = v[0:1] + v[2:3] + v[4:5]
        high = v[1:2] + v[3:4] + v[5:6]
        variance[k : k + 1, at] = dvar[k : k + 1, at] + low_high(turned(low), high)
    for m in range(nj // 2):
        at = slice(m * LANES, (m + 1) * LANES)
        a = got[2 * m, rt : rt + rp, :].astype(F32)
        b = got[2 * m + 1, rt : rt + rp, :].astype(F32)
        cross_par[:, at] = jnp.concatenate(
            [low_high(a, turned(b)), low_high(turned(a), b)], axis=0
        ).astype(BF16)
        a = got[2 * m, rt + 2 * rp : rt + 3 * rp, :].astype(F32)
        b = got[2 * m + 1, rt + 2 * rp : rt + 3 * rp, :].astype(F32)
        sigma_par[:, at] = (dinv[:, at] + low_high(a, turned(b))).astype(BF16)


def device_part(
    sigma_top,
    panel_par,
    dinv_par,
    panel_kid_top,
    panel_kid_par,
    dvar_kid,
    mask_par,
    mask_kid_top,
    mask_kid_par,
):
    rt, wt = sigma_top.shape
    rp, w1 = dinv_par.shape
    kids, _, w2 = panel_kid_top.shape
    ny = lax.axis_size("y")
    nx = lax.axis_size("x")
    nj = lax.axis_size(XC)
    assert kids * w2 == nj * LANES and w1 == nj * HALF and wt == 2 * w1
    assert nx == 8 and rt == 2 * rp and nj * rp == LANES and ny * LANES == w1

    def fetching(kernel, outs, arrays):
        return call(
            kernel,
            outs,
            tuple(pltpu.with_memory_space_constraint(a, pltpu.HBM) for a in arrays),
            [pl.BlockSpec(memory_space=pltpu.HBM)] * len(arrays),
            [pltpu.VMEM(a.shape, a.dtype) for a in arrays]
            + [pltpu.SemaphoreType.DMA((len(arrays),))],
        )

    masks = (mask_par.T, mask_kid_top.transpose(0, 2, 1), mask_kid_par)
    (slots,) = fetching(
        slots_kernel,
        [((nj, 2 * rp + rt, LANES), BF16)],
        (panel_par, panel_kid_top, panel_kid_par, *masks),
    )
    cols = exchanged(slots, XC)
    (rows,) = fetching(
        rows_kernel,
        [((3 * rt + rp, w1), BF16)],
        (sigma_top, panel_par, dinv_par, masks[0]),
    )
    far_rows = swapped(rows, "x", 4)
    (dvar_kid,) = fetching(copy_kernel, [(dvar_kid.shape, F32)], (dvar_kid,))
    par_rows, rows = call(
        stack_kernel,
        [((2, rt, w1), BF16), ((2, 2 * rt + rp, w1), BF16)],
        (rows, far_rows),
    )
    (tall_send,) = call(repeat_kernel, [((ny, nj, 2 * rp, LANES), BF16)], (cols,))
    tall = exchanged(tall_send, "y")
    par_rows = jnp.concatenate([par_rows, swapped(par_rows, "x", 2)])
    par_own = jnp.concatenate([par_rows, swapped(par_rows, "x", 1)])
    par_other = swapped(par_own, "c", 1)
    rows_2 = swapped(rows, "x", 2)
    (rows,) = call(join_kernel, [((4, 2 * rt + rp, w1), BF16)], (rows, rows_2))
    near = jnp.concatenate([rows, swapped(rows, "x", 1)])
    far = swapped(near, "c", 1)

    def sized(kernel):
        return lambda *refs: kernel(rt, rp, *refs)

    send, step = call(
        sized(step_kernel),
        [((ny, nj, rt, LANES), BF16), ((nj, rt, LANES), F32)],
        (cols, tall, par_own, par_other),
    )
    step_j = exchanged(send, "y")
    rows4 = nj * rp + nj * rp // 2 + 8
    slots4, part, db = call(
        sized(main_kernel),
        [((ny, rows4, LANES), BF16), ((nj, rt + rp, LANES), BF16), ((nj, rp, LANES), F32)],
        (near, far, par_own, par_other, tall, step_j, cols, step),
    )
    received = exchanged(slots4, "y")
    (out,) = call(
        sized(sum_kernel), [((nj, rt + 3 * rp, LANES), BF16)], (received, db, part)
    )
    got = exchanged(out, XC)
    return call(
        sized(final_kernel),
        [
            ((rt, w1), BF16),
            ((rp, w1), BF16),
            ((kids, rt, w2), BF16),
            ((kids, rp, w2), BF16),
            ((kids, w2), F32),
        ],
        (got, dinv_par, dvar_kid),
    )


def solution(mesh):
    finer = Mesh(mesh.devices.reshape(mesh.shape["parts"], 8, 8, 2), PARTS_ROW)
    return jax.shard_map(
        device_part,
        mesh=finer,
        in_specs=(
            P(PARTS_ROW, None),
            P(PARTS_ROW, None),
            P(PARTS_ROW, None),
            P("parts", ROW, None),
            P("parts", ROW, None),
            P("parts", None),
            P("parts", None),
            P("parts", None, None),
            P("parts", None, None),
        ),
        out_specs=(
            P(PARTS_ROW, None),
            P(PARTS_ROW, None),
            P("parts", ROW, None),
            P("parts", ROW, None),
            P("parts", None),
        ),
        check_vma=False,
    )
```

```python
import jax
import jax.numpy as jnp
from jax import lax
from jax.experimental import pallas as pl
from jax.experimental.pallas import tpu as pltpu
from jax.sharding import Mesh
from jax.sharding import PartitionSpec as P

BLK = 256
LANES = 128
HALF = LANES // 2
ROW = ("y", "x", "c")
PARTS_ROW = ("parts", "y", "x", "c")
XC = ("x", "c")
F32 = jnp.float32
BF16 = jnp.bfloat16
VMEM = pl.BlockSpec(memory_space=pltpu.VMEM)
SMEM = pl.BlockSpec(memory_space=pltpu.SMEM)


def exchanged(x, axes):
    return lax.all_to_all(x, axes, split_axis=0, concat_axis=0, tiled=True)


def swapped(x, axis, bit):
    return lax.ppermute(x, axis, [(i, i ^ bit) for i in range(lax.axis_size(axis))])


def dot(a, b):
    return jnp.dot(a, b, preferred_element_type=F32)


def dot_t(a, b):
    return lax.dot_general(a, b, (((0,), (0,)), ((), ())), preferred_element_type=F32)


def turned(x):
    return pltpu.roll(x, HALF, x.ndim - 1)


def low_high(low, high):
    lane = lax.broadcasted_iota(jnp.int32, low.shape, low.ndim - 1)
    return jnp.where(lane < HALF, low, high)


def split3(v):
    parts = []
    for _ in range(3):
        top = v.astype(BF16).astype(F32)
        parts.append(top)
        v = v - top
    return parts


def call(kernel, outs, args, specs=None, scratch=()):
    return pl.pallas_call(
        kernel,
        out_shape=tuple(jax.ShapeDtypeStruct(s, d) for s, d in outs),
        in_specs=specs or [VMEM] * len(args),
        out_specs=tuple(VMEM for _ in outs),
        scratch_shapes=scratch,
        compiler_params=pltpu.CompilerParams(vmem_limit_bytes=48 * 2**20),
    )(*args)


def fetched(sources, scratch, done):
    pairs = enumerate(zip(sources, scratch))
    copies = [pltpu.make_async_copy(a, b, done.at[i]) for i, (a, b) in pairs]
    for copy in copies:
        copy.start()
    for copy in copies:
        copy.wait()


def lane_of(mask, at):
    lane = lax.broadcasted_iota(jnp.int32, mask.shape, 1)
    return jnp.sum(jnp.where(lane == at, mask, 0).astype(F32), axis=1, keepdims=True)


def slots_kernel(*refs):
    sources, slots, scratch, done = refs[:6], refs[6], refs[7:13], refs[13]
    fetched(sources, scratch, done)
    par, kid_top, kid_par, mask_par, mask_kid_top, mask_kid_par = scratch
    rt, w1 = par.shape
    kids, rp = kid_par.shape[:2]
    nj = slots.shape[0]
    position = lax.axis_index(ROW)
    block_top = lax.div(position * rt, BLK)
    block_par = lax.div(position * rp, BLK)
    keep = lane_of(mask_par[...], block_top)
    packed = []
    for m in range(w1 // LANES):
        at = slice(m * LANES, (m + 1) * LANES)
        block = m * LANES // BLK
        piece = par[:, at].astype(F32) * keep[block : block + 1]
        top, low = piece[:rp], piece[rp:]
        packed.append(low_high(top, turned(low)))
        packed.append(low_high(turned(top), low))
    per_kid = nj // kids
    for k in range(kids):
        keep_top = lane_of(mask_kid_top[k], block_top)
        keep_par = mask_kid_par[k, pl.ds(block_par, 1), :].astype(F32)
        for m in range(per_kid):
            j = k * per_kid + m
            at = slice(m * LANES, (m + 1) * LANES)
            block = m * LANES // BLK
            piece = kid_par[k, :, at].astype(F32) * keep_par[:, block : block + 1]
            slots[j, 0 : 2 * rp, :] = jnp.concatenate([piece, packed[j]], axis=0).astype(BF16)
            piece = kid_top[k, :, at].astype(F32) * keep_top[block : block + 1]
            slots[j, 2 * rp : 2 * rp + rt, :] = piece.astype(BF16)


def rows_kernel(*refs):
    sources, rows, scratch, done = refs[:4], refs[4], refs[5:9], refs[9]
    fetched(sources, scratch, done)
    sigma, par, dinv, mask_par = scratch
    rt, w1 = par.shape
    rp = dinv.shape[0]
    keep = lane_of(mask_par[...], lax.div(lax.axis_index(ROW) * rt, BLK))
    for b in range(w1 // BLK):
        at = slice(b * BLK, (b + 1) * BLK)
        rows[0:rt, at] = (par[:, at].astype(F32) * keep[b : b + 1]).astype(BF16)
    rows[rt : 2 * rt, :] = sigma[:, 0:w1]
    rows[2 * rt : 3 * rt, :] = sigma[:, w1 : 2 * w1]
    rows[3 * rt : 3 * rt + rp, :] = dinv[...].astype(BF16)


def copy_kernel(source_hbm, result, scratch, done):
    fetched((source_hbm,), (scratch,), done)
    result[...] = scratch[...]


def stack_kernel(own, other, par_rows, rows):
    rt = par_rows.shape[1]
    for i, source in enumerate((own, other)):
        par_rows[i] = source[0:rt, :]
        rows[i] = source[rt : rt + rows.shape[1], :]


def join_kernel(own, other, joined):
    count = own.shape[0]
    joined[0:count] = own[...]
    joined[count : 2 * count] = other[...]


def repeat_kernel(cols, send):
    rows = send.shape[2]
    for y in range(send.shape[0]):
        send[y] = cols[:, 0:rows, :]


def kid_par_columns(tall):
    ny, nj, rows, _ = tall.shape
    rp = rows // 2
    return tall[:, :, 0:rp, :].astype(F32).reshape(ny * nj * rp, LANES).astype(BF16)


def chunk_place(x_me, c_me, bits):
    b1, b2, b4, bc = bits
    return 2 * jnp.bitwise_xor(x_me, b1 + 2 * b2 + 4 * b4) + jnp.bitwise_xor(c_me, bc)


def step_kernel(rt, rp, cols, tall, par_own, par_other, send, step):
    x_me, c_me = lax.axis_index("x"), lax.axis_index("c")
    kid_par_j = kid_par_columns(tall)
    for bc, par in enumerate((par_own, par_other)):
        count, _, w1 = par.shape
        product = dot(par[...].reshape(count * rt, w1), kid_par_j)
        for k in range(count):
            at = chunk_place(x_me, c_me, (k // 4, (k // 2) % 2, k % 2, bc))
            total = cols[at, 2 * rp : 2 * rp + rt, :].astype(F32) + product[k * rt : (k + 1) * rt]
            step[at] = total
            rounded = total.astype(BF16)
            for y in range(send.shape[0]):
                send[y, at] = rounded


def main_kernel(
    near, far, par_own, par_other, tall, step_j, cols, step, slots, part_near, part_far, db
):
    count, _, w1 = near.shape
    ny, nj = tall.shape[:2]
    rt = par_own.shape[1]
    rp = rt // 2
    x_me, c_me = lax.axis_index("x"), lax.axis_index("c")
    kid_par_j = kid_par_columns(tall)
    par_j = tall[:, :, rp : 2 * rp, :].astype(F32).reshape(ny * nj, 1, rp, LANES)
    par_j = jnp.concatenate([par_j, turned(par_j)], axis=1)
    par_j = par_j.reshape(ny * nj * 2 * rp, LANES).astype(BF16)
    both = jnp.concatenate([step_j[...].reshape(ny * nj * rt, LANES), par_j], axis=1)

    var = jnp.zeros((1, LANES), F32)
    xs = []
    for bc, chunks in enumerate((near, far)):
        s0 = chunks[:, 0:rt, :].reshape(count * rt, w1)
        s1 = chunks[:, rt : 2 * rt, :].reshape(count * rt, w1)
        d = chunks[:, 2 * rt : 2 * rt + rp, :].astype(F32).reshape(count * rp, w1)
        x = dot(s0, both[:w1]) + dot(s1, both[w1:])
        db_own = dot(d.astype(BF16), kid_par_j)
        for k in range(count):
            b1, b2, b4 = k // 4, (k // 2) % 2, k % 2
            at = chunk_place(x_me, c_me, (b1, b2, b4, bc))
            part, to = (part_near, part_far)[b4], 4 * b2 + 2 * b1 + bc
            piece = x[k * rt : (k + 1) * rt]
            kt = piece[:, :LANES].astype(BF16)
            part[to, 0:rt, :] = kt
            c = piece[:, LANES:]
            part[to, rt : rt + rp, :] = low_high(c[:rp], turned(c[rp:])).astype(BF16)
            db_k = db_own[k * rp : (k + 1) * rp]
            db[at] = db_k
            var = var + jnp.sum(step[at] * kt.astype(F32), axis=0, keepdims=True)
            var = var + jnp.sum(cols[at, 0:rp, :].astype(F32) * db_k, axis=0, keepdims=True)
        xs.append(x.astype(BF16))

    x = jnp.concatenate(xs, axis=0)
    p = jnp.concatenate([p[...].reshape(nj // 2 * rt, w1) for p in (par_own, par_other)], axis=0)
    var_rows = jnp.concatenate(split3(var) + [jnp.zeros((rp - 3, LANES), F32)], axis=0)
    db_here = db[...].reshape(nj * rp, LANES)
    nx = nj // 2
    for y in range(ny):
        partial = dot_t(p[:, y * LANES : (y + 1) * LANES], x)
        kp = partial[:, :LANES] + jnp.where(lax.axis_index("y") == y, db_here, 0.0)
        for i in range(nx):
            slots[y * nx + i, 0:rt, :] = kp[i * rt : (i + 1) * rt].astype(BF16)
            q = partial[i * rt : (i + 1) * rt, LANES:]
            q = low_high(q[:rp], turned(q[rp:]))
            slots[y * nx + i, rt : 2 * rt, :] = jnp.concatenate([q, var_rows], axis=0).astype(BF16)


def top_kernel(own, other, kid_top, cross_par):
    count, rows, _ = own.shape
    rp = rows // 3
    rt = 2 * rp
    kids = kid_top.shape[0]
    per_kid = 2 * count // kids
    x_me, c_me = lax.axis_index("x"), lax.axis_index("c")
    first = c_me == 0
    for k in range(count):
        chip = jnp.bitwise_xor(x_me, k // 4 + 2 * ((k // 2) % 2) + 4 * (k % 2))
        a = jnp.where(first, own[k], other[k])
        b = jnp.where(first, other[k], own[k])
        kid = lax.div(2 * chip, per_kid)
        block = lax.rem(2 * chip, per_kid)
        for i, slot in enumerate((a, b)):
            at = pl.ds(pl.multiple_of((block + i) * LANES, LANES), LANES)
            kid_top[kid, :, at] = slot[0:rt]
        a, b = a[rt:].astype(F32), b[rt:].astype(F32)
        at = pl.ds(pl.multiple_of(chip * LANES, LANES), LANES)
        c = jnp.concatenate([low_high(a, turned(b)), low_high(turned(a), b)], axis=0)
        cross_par[:, at] = c.astype(BF16)


def sum_kernel(received, keep, send):
    nx = keep.shape[0]
    rp = keep.shape[1] // 2
    first = lax.axis_index("c") == 0
    for i in range(nx):
        total = received[i].astype(F32)
        for y in range(1, received.shape[0] // nx):
            total = total + received[y * nx + i].astype(F32)
        kp_0, kp_1 = total[:rp], total[rp : 2 * rp]
        q_0 = total[2 * rp : 3 * rp]
        q_1 = turned(q_0)
        var = total[3 * rp : 3 * rp + 1] + total[3 * rp + 1 : 3 * rp + 2]
        var = var + total[3 * rp + 2 : 3 * rp + 3]
        var_rows = []
        for top in split3(var):
            var_rows += [turned(top), top]
        var_rows = jnp.concatenate(var_rows + [jnp.zeros((2, LANES), F32)], axis=0)
        low = jnp.concatenate([kp_0, low_high(q_0, var_rows)], axis=0)
        high = jnp.concatenate([kp_1, low_high(q_1, var_rows)], axis=0)
        keep[i] = jnp.where(first, low, high).astype(BF16)
        send[i] = jnp.where(first, high, low).astype(BF16)


def final_kernel(keep, got, dinv, dvar, sigma_par, kid_par, variance):
    nx = keep.shape[0]
    rp = dinv.shape[0]
    kids = dvar.shape[0]
    per_kid = 2 * nx // kids
    first = lax.axis_index("c") == 0
    for i in range(nx):
        mine, others = keep[i].astype(F32), got[i].astype(F32)
        a = jnp.where(first, mine, others)
        b = jnp.where(first, others, mine)
        for j, slot in ((2 * i, a), (2 * i + 1, b)):
            k, m = divmod(j, per_kid)
            at = slice(m * LANES, (m + 1) * LANES)
            kid_par[k, :, at] = slot[:rp].astype(BF16)
            v = slot[rp:]
            low = v[0:1] + v[2:3] + v[4:5]
            high = v[1:2] + v[3:4] + v[5:6]
            variance[k : k + 1, at] = dvar[k : k + 1, at] + low_high(turned(low), high)
        at = slice(i * LANES, (i + 1) * LANES)
        sigma_par[:, at] = (dinv[:, at] + low_high(a[rp:], turned(b[rp:]))).astype(BF16)


def device_part(
    sigma_top,
    panel_par,
    dinv_par,
    panel_kid_top,
    panel_kid_par,
    dvar_kid,
    mask_par,
    mask_kid_top,
    mask_kid_par,
):
    rt, wt = sigma_top.shape
    rp, w1 = dinv_par.shape
    kids, _, w2 = panel_kid_top.shape
    ny = lax.axis_size("y")
    nx = lax.axis_size("x")
    nj = lax.axis_size(XC)
    assert kids * w2 == nj * LANES and w1 == nj * HALF and wt == 2 * w1
    assert nx == 8 and rt == 2 * rp and nj * rp == LANES and ny * LANES == w1

    def fetching(kernel, outs, arrays):
        return call(
            kernel,
            outs,
            tuple(pltpu.with_memory_space_constraint(a, pltpu.HBM) for a in arrays),
            [pl.BlockSpec(memory_space=pltpu.HBM)] * len(arrays),
            [pltpu.VMEM(a.shape, a.dtype) for a in arrays]
            + [pltpu.SemaphoreType.DMA((len(arrays),))],
        )

    masks = (mask_par.T, mask_kid_top.transpose(0, 2, 1), mask_kid_par)
    (slots,) = fetching(
        slots_kernel,
        [((nj, 2 * rp + rt, LANES), BF16)],
        (panel_par, panel_kid_top, panel_kid_par, *masks),
    )
    cols = exchanged(slots, XC)
    (rows,) = fetching(
        rows_kernel,
        [((3 * rt + rp, w1), BF16)],
        (sigma_top, panel_par, dinv_par, masks[0]),
    )
    far_rows = swapped(rows, "x", 4)
    (dvar_kid,) = fetching(copy_kernel, [(dvar_kid.shape, F32)], (dvar_kid,))
    par_rows, rows = call(
        stack_kernel,
        [((2, rt, w1), BF16), ((2, 2 * rt + rp, w1), BF16)],
        (rows, far_rows),
    )
    (tall_send,) = call(repeat_kernel, [((ny, nj, 2 * rp, LANES), BF16)], (cols,))
    tall = exchanged(tall_send, "y")
    par_rows = jnp.concatenate([par_rows, swapped(par_rows, "x", 2)])
    par_own = jnp.concatenate([par_rows, swapped(par_rows, "x", 1)])
    par_other = swapped(par_own, "c", 1)
    rows_2 = swapped(rows, "x", 2)
    (rows,) = call(join_kernel, [((4, 2 * rt + rp, w1), BF16)], (rows, rows_2))
    near = jnp.concatenate([rows, swapped(rows, "x", 1)])
    far = swapped(near, "c", 1)

    def sized(kernel):
        return lambda *refs: kernel(rt, rp, *refs)

    send, step = call(
        sized(step_kernel),
        [((ny, nj, rt, LANES), BF16), ((nj, rt, LANES), F32)],
        (cols, tall, par_own, par_other),
    )
    step_j = exchanged(send, "y")
    slot = (rt + rp, LANES)
    slots, part_near, part_far = call(
        main_kernel,
        [((ny * nx, 2 * rt, LANES), BF16), ((nj // 2, *slot), BF16), ((nj // 2, *slot), BF16)],
        (near, far, par_own, par_other, tall, step_j, cols, step),
        scratch=[pltpu.VMEM((nj, rp, LANES), F32)],
    )
    received = exchanged(slots, ("y", "x"))
    got = swapped(part_far, "x", 4)
    held = jnp.stack([part_near, got]).reshape(2, 2, 4, *slot)
    got = swapped(held[:, 1], "x", 2)
    held = jnp.stack([held[:, 0], got]).reshape(2, 2, 2, 2, *slot)
    got = swapped(held[:, :, 1], "x", 1)
    held = jnp.stack([held[:, :, 0], got])
    got = swapped(held[:, :, :, 1], "c", 1)
    own = held[:, :, :, 0].reshape(nj // 2, *slot)
    cross_kid_top, cross_par = call(
        top_kernel,
        [((kids, rt, w2), BF16), ((rt, w1), BF16)],
        (own, got.reshape(nj // 2, *slot)),
    )
    keep, send = call(sum_kernel, [((nx, rt, LANES), BF16)] * 2, (received,))
    got = swapped(send, "c", 1)
    sigma_par, cross_kid_par, variance_kid = call(
        final_kernel,
        [((rp, w1), BF16), ((kids, rp, w2), BF16), ((kids, w2), F32)],
        (keep, got, dinv_par, dvar_kid),
    )
    return cross_par, sigma_par, cross_kid_top, cross_kid_par, variance_kid


def solution(mesh):
    finer = Mesh(mesh.devices.reshape(mesh.shape["parts"], 8, 8, 2), PARTS_ROW)
    return jax.shard_map(
        device_part,
        mesh=finer,
        in_specs=(
            P(PARTS_ROW, None),
            P(PARTS_ROW, None),
            P(PARTS_ROW, None),
            P("parts", ROW, None),
            P("parts", ROW, None),
            P("parts", None),
            P("parts", None),
            P("parts", None, None),
            P("parts", None, None),
        ),
        out_specs=(
            P(PARTS_ROW, None),
            P(PARTS_ROW, None),
            P("parts", ROW, None),
            P("parts", ROW, None),
            P("parts", None),
        ),
        check_vma=False,
    )
```

```python
import jax
import jax.numpy as jnp
from jax import lax
from jax.experimental import pallas as pl
from jax.experimental.pallas import tpu as pltpu
from jax.sharding import Mesh
from jax.sharding import PartitionSpec as P

BLK = 256
LANES = 128
HALF = LANES // 2
ROW = ("y", "x", "c")
PARTS_ROW = ("parts", "y", "x", "c")
XC = ("x", "c")
F32 = jnp.float32
BF16 = jnp.bfloat16
VMEM = pl.BlockSpec(memory_space=pltpu.VMEM)
SMEM = pl.BlockSpec(memory_space=pltpu.SMEM)


def exchanged(x, axes):
    return lax.all_to_all(x, axes, split_axis=0, concat_axis=0, tiled=True)


def swapped(x, axis, bit):
    return lax.ppermute(x, axis, [(i, i ^ bit) for i in range(lax.axis_size(axis))])


def dot(a, b):
    return jnp.dot(a, b, preferred_element_type=F32)


def dot_t(a, b):
    return lax.dot_general(a, b, (((0,), (0,)), ((), ())), preferred_element_type=F32)


def turned(x):
    return pltpu.roll(x, HALF, x.ndim - 1)


def low_high(low, high):
    lane = lax.broadcasted_iota(jnp.int32, low.shape, low.ndim - 1)
    return jnp.where(lane < HALF, low, high)


def split3(v):
    parts = []
    for _ in range(3):
        top = v.astype(BF16).astype(F32)
        parts.append(top)
        v = v - top
    return parts


def call(kernel, outs, args, specs=None, scratch=()):
    return pl.pallas_call(
        kernel,
        out_shape=tuple(jax.ShapeDtypeStruct(s, d) for s, d in outs),
        in_specs=specs or [VMEM] * len(args),
        out_specs=tuple(VMEM for _ in outs),
        scratch_shapes=scratch,
        compiler_params=pltpu.CompilerParams(vmem_limit_bytes=48 * 2**20),
    )(*args)


def fetched(sources, scratch, done):
    pairs = enumerate(zip(sources, scratch))
    copies = [pltpu.make_async_copy(a, b, done.at[i]) for i, (a, b) in pairs]
    for copy in copies:
        copy.start()
    for copy in copies:
        copy.wait()


def lane_of(mask, at):
    lane = lax.broadcasted_iota(jnp.int32, mask.shape, 1)
    return jnp.sum(jnp.where(lane == at, mask, 0).astype(F32), axis=1, keepdims=True)


def slots_kernel(*refs):
    sources, slots, scratch, done = refs[:6], refs[6], refs[7:13], refs[13]
    fetched(sources, scratch, done)
    par, kid_top, kid_par, mask_par, mask_kid_top, mask_kid_par = scratch
    rt, w1 = par.shape
    kids, rp = kid_par.shape[:2]
    nj = slots.shape[0]
    position = lax.axis_index(ROW)
    block_top = lax.div(position * rt, BLK)
    block_par = lax.div(position * rp, BLK)
    keep = lane_of(mask_par[...], block_top)
    packed = []
    for m in range(w1 // LANES):
        at = slice(m * LANES, (m + 1) * LANES)
        block = m * LANES // BLK
        piece = par[:, at].astype(F32) * keep[block : block + 1]
        top, low = piece[:rp], piece[rp:]
        packed.append(low_high(top, turned(low)))
        packed.append(low_high(turned(top), low))
    per_kid = nj // kids
    for k in range(kids):
        keep_top = lane_of(mask_kid_top[k], block_top)
        keep_par = mask_kid_par[k, pl.ds(block_par, 1), :].astype(F32)
        for m in range(per_kid):
            j = k * per_kid + m
            at = slice(m * LANES, (m + 1) * LANES)
            block = m * LANES // BLK
            piece = kid_par[k, :, at].astype(F32) * keep_par[:, block : block + 1]
            slots[j, 0 : 2 * rp, :] = jnp.concatenate([piece, packed[j]], axis=0).astype(BF16)
            piece = kid_top[k, :, at].astype(F32) * keep_top[block : block + 1]
            slots[j, 2 * rp : 2 * rp + rt, :] = piece.astype(BF16)


def rows_kernel(*refs):
    sources, rows, scratch, done = refs[:4], refs[4], refs[5:9], refs[9]
    fetched(sources, scratch, done)
    sigma, par, dinv, mask_par = scratch
    rt, w1 = par.shape
    rp = dinv.shape[0]
    keep = lane_of(mask_par[...], lax.div(lax.axis_index(ROW) * rt, BLK))
    for b in range(w1 // BLK):
        at = slice(b * BLK, (b + 1) * BLK)
        rows[0:rt, at] = (par[:, at].astype(F32) * keep[b : b + 1]).astype(BF16)
    rows[rt : 2 * rt, :] = sigma[:, 0:w1]
    rows[2 * rt : 3 * rt, :] = sigma[:, w1 : 2 * w1]
    rows[3 * rt : 3 * rt + rp, :] = dinv[...].astype(BF16)


def copy_kernel(source_hbm, result, scratch, done):
    fetched((source_hbm,), (scratch,), done)
    result[...] = scratch[...]


def stack_kernel(own, other, par_rows, rows):
    rt = par_rows.shape[1]
    for i, source in enumerate((own, other)):
        par_rows[i] = source[0:rt, :]
        rows[i] = source[rt : rt + rows.shape[1], :]


def join_kernel(own, other, joined):
    count = own.shape[0]
    joined[0:count] = own[...]
    joined[count : 2 * count] = other[...]


def repeat_kernel(cols, send):
    rows = send.shape[2]
    for y in range(send.shape[0]):
        send[y] = cols[:, 0:rows, :]


def kid_par_columns(tall):
    ny, nj, rows, _ = tall.shape
    rp = rows // 2
    return tall[:, :, 0:rp, :].astype(F32).reshape(ny * nj * rp, LANES).astype(BF16)


def chunk_place(x_me, c_me, bits):
    b1, b2, b4, bc = bits
    return 2 * jnp.bitwise_xor(x_me, b1 + 2 * b2 + 4 * b4) + jnp.bitwise_xor(c_me, bc)


def step_kernel(rt, rp, cols, tall, par_own, par_other, rounded, step):
    x_me, c_me = lax.axis_index("x"), lax.axis_index("c")
    kid_par_j = kid_par_columns(tall)
    for bc, par in enumerate((par_own, par_other)):
        count, _, w1 = par.shape
        product = dot(par[...].reshape(count * rt, w1), kid_par_j)
        for k in range(count):
            at = chunk_place(x_me, c_me, (k // 4, (k // 2) % 2, k % 2, bc))
            total = cols[at, 2 * rp : 2 * rp + rt, :].astype(F32) + product[k * rt : (k + 1) * rt]
            step[at] = total
            rounded[at] = total.astype(BF16)


def main_kernel(rt, rp, near, far, par_own, par_other, tall, cols, step, *refs):
    steps, (slots, part, db, step_j) = refs[:-4], refs[-4:]
    for k, rows in enumerate(steps):
        step_j[jnp.bitwise_xor(lax.axis_index("y"), k)] = rows[...]
    w1 = near.shape[-1]
    ny, nj = tall.shape[:2]
    x_me, c_me = lax.axis_index("x"), lax.axis_index("c")
    kid_par_j = kid_par_columns(tall)
    par_j = tall[:, :, rp : 2 * rp, :].astype(F32).reshape(ny * nj, 1, rp, LANES)
    par_j = jnp.concatenate([par_j, turned(par_j)], axis=1)
    par_j = par_j.reshape(ny * nj * 2 * rp, LANES).astype(BF16)
    both = jnp.concatenate([step_j[...].reshape(ny * nj * rt, LANES), par_j], axis=1)

    var = jnp.zeros((1, LANES), F32)
    xs = []
    for bc, chunks in enumerate((near, far)):
        count = chunks.shape[0]
        s0 = chunks[:, 0:rt, :].reshape(count * rt, w1)
        s1 = chunks[:, rt : 2 * rt, :].reshape(count * rt, w1)
        d = chunks[:, 2 * rt : 2 * rt + rp, :].astype(F32).reshape(count * rp, w1)
        x = dot(s0, both[:w1]) + dot(s1, both[w1:])
        db_own = dot(d.astype(BF16), kid_par_j)
        for k in range(count):
            at = chunk_place(x_me, c_me, (k // 4, (k // 2) % 2, k % 2, bc))
            piece = x[k * rt : (k + 1) * rt]
            kt = piece[:, :LANES].astype(BF16)
            part[at, 0:rt, :] = kt
            c = piece[:, LANES:]
            part[at, rt : rt + rp, :] = low_high(c[:rp], turned(c[rp:])).astype(BF16)
            db_k = db_own[k * rp : (k + 1) * rp]
            db[at] = db_k
            var = var + jnp.sum(step[at] * kt.astype(F32), axis=0, keepdims=True)
            var = var + jnp.sum(cols[at, 0:rp, :].astype(F32) * db_k, axis=0, keepdims=True)
        xs.append(x.astype(BF16))

    x = jnp.concatenate(xs, axis=0)
    p = jnp.concatenate([p[...].reshape(nj // 2 * rt, w1) for p in (par_own, par_other)], axis=0)
    for y in range(ny):
        partial = dot_t(p[:, y * LANES : (y + 1) * LANES], x)
        rows = partial.shape[0]
        slots[y, 0:rows, :] = partial[:, :LANES].astype(BF16)
        q = partial[:, LANES:]
        q = low_high(q[: rows // 2], turned(q[rows // 2 :]))
        slots[y, rows : rows + rows // 2, :] = q.astype(BF16)
    var_rows = jnp.concatenate(split3(var) + [jnp.zeros((5, LANES), F32)], axis=0).astype(BF16)
    for y in range(ny):
        slots[y, rows + rows // 2 : rows + rows // 2 + 8, :] = var_rows


def sum_kernel(rt, rp, received, db, part, out):
    ny = received.shape[0]
    nj = out.shape[0]
    rows = nj * rp
    total = received[0].astype(F32)
    for y in range(1, ny):
        total = total + received[y].astype(F32)
    q = total[rows : rows + rows // 2]
    q = jnp.concatenate([q, turned(q)], axis=0)
    first = rows + rows // 2
    var = total[first : first + 1] + total[first + 1 : first + 2] + total[first + 2 : first + 3]
    var_rows = []
    for top in split3(var):
        var_rows += [turned(top), top]
    var_rows = jnp.concatenate(var_rows + [jnp.zeros((2, LANES), F32)], axis=0)
    for j in range(nj):
        at = slice(j * rp, (j + 1) * rp)
        out[j, 0 : rt + rp, :] = part[j]
        kp = total[at] + db[j]
        out[j, rt + rp : rt + 3 * rp, :] = jnp.concatenate(
            [kp, low_high(q[at], var_rows)], axis=0
        ).astype(BF16)


def final_kernel(rt, rp, got, dinv, dvar, cross_par, sigma_par, kid_top, kid_par, variance):
    nj = got.shape[0]
    kids = dvar.shape[0]
    per_kid = nj // kids
    for j in range(nj):
        k, m = divmod(j, per_kid)
        at = slice(m * LANES, (m + 1) * LANES)
        kid_top[k, :, at] = got[j, 0:rt, :]
        kid_par[k, :, at] = got[j, rt + rp : rt + 2 * rp, :]
        v = got[j, rt + 2 * rp : rt + 3 * rp, :].astype(F32)
        low = v[0:1] + v[2:3] + v[4:5]
        high = v[1:2] + v[3:4] + v[5:6]
        variance[k : k + 1, at] = dvar[k : k + 1, at] + low_high(turned(low), high)
    for m in range(nj // 2):
        at = slice(m * LANES, (m + 1) * LANES)
        a = got[2 * m, rt : rt + rp, :].astype(F32)
        b = got[2 * m + 1, rt : rt + rp, :].astype(F32)
        cross_par[:, at] = jnp.concatenate(
            [low_high(a, turned(b)), low_high(turned(a), b)], axis=0
        ).astype(BF16)
        a = got[2 * m, rt + 2 * rp : rt + 3 * rp, :].astype(F32)
        b = got[2 * m + 1, rt + 2 * rp : rt + 3 * rp, :].astype(F32)
        sigma_par[:, at] = (dinv[:, at] + low_high(a, turned(b))).astype(BF16)


def device_part(
    sigma_top,
    panel_par,
    dinv_par,
    panel_kid_top,
    panel_kid_par,
    dvar_kid,
    mask_par,
    mask_kid_top,
    mask_kid_par,
):
    rt, wt = sigma_top.shape
    rp, w1 = dinv_par.shape
    kids, _, w2 = panel_kid_top.shape
    ny = lax.axis_size("y")
    nx = lax.axis_size("x")
    nj = lax.axis_size(XC)
    assert kids * w2 == nj * LANES and w1 == nj * HALF and wt == 2 * w1
    assert nx == 8 and rt == 2 * rp and nj * rp == LANES and ny * LANES == w1

    def fetching(kernel, outs, arrays):
        return call(
            kernel,
            outs,
            tuple(pltpu.with_memory_space_constraint(a, pltpu.HBM) for a in arrays),
            [pl.BlockSpec(memory_space=pltpu.HBM)] * len(arrays),
            [pltpu.VMEM(a.shape, a.dtype) for a in arrays]
            + [pltpu.SemaphoreType.DMA((len(arrays),))],
        )

    masks = (mask_par.T, mask_kid_top.transpose(0, 2, 1), mask_kid_par)
    (slots,) = fetching(
        slots_kernel,
        [((nj, 2 * rp + rt, LANES), BF16)],
        (panel_par, panel_kid_top, panel_kid_par, *masks),
    )
    cols = exchanged(slots, XC)
    (rows,) = fetching(
        rows_kernel,
        [((3 * rt + rp, w1), BF16)],
        (sigma_top, panel_par, dinv_par, masks[0]),
    )
    far_rows = swapped(rows, "x", 4)
    (dvar_kid,) = fetching(copy_kernel, [(dvar_kid.shape, F32)], (dvar_kid,))
    par_rows, rows = call(
        stack_kernel,
        [((2, rt, w1), BF16), ((2, 2 * rt + rp, w1), BF16)],
        (rows, far_rows),
    )
    (tall_send,) = call(repeat_kernel, [((ny, nj, 2 * rp, LANES), BF16)], (cols,))
    tall = exchanged(tall_send, "y")
    par_rows = jnp.concatenate([par_rows, swapped(par_rows, "x", 2)])
    par_own = jnp.concatenate([par_rows, swapped(par_rows, "x", 1)])
    par_other = swapped(par_own, "c", 1)
    rows_2 = swapped(rows, "x", 2)
    (rows,) = call(join_kernel, [((4, 2 * rt + rp, w1), BF16)], (rows, rows_2))
    near = jnp.concatenate([rows, swapped(rows, "x", 1)])
    far = swapped(near, "c", 1)

    def sized(kernel):
        return lambda *refs: kernel(rt, rp, *refs)

    rounded, step = call(
        sized(step_kernel),
        [((nj, rt, LANES), BF16), ((nj, rt, LANES), F32)],
        (cols, tall, par_own, par_other),
    )
    steps = [rounded]
    for k in range(1, ny):
        steps.append(swapped(rounded, "y", k))
    rows4 = nj * rp + nj * rp // 2 + 8
    slots4, part, db = call(
        sized(main_kernel),
        [((ny, rows4, LANES), BF16), ((nj, rt + rp, LANES), BF16), ((nj, rp, LANES), F32)],
        (near, far, par_own, par_other, tall, cols, step, *steps),
        scratch=[pltpu.VMEM((ny, nj, rt, LANES), BF16)],
    )
    received = exchanged(slots4, "y")
    (out,) = call(
        sized(sum_kernel), [((nj, rt + 3 * rp, LANES), BF16)], (received, db, part)
    )
    got = exchanged(out, XC)
    return call(
        sized(final_kernel),
        [
            ((rt, w1), BF16),
            ((rp, w1), BF16),
            ((kids, rt, w2), BF16),
            ((kids, rp, w2), BF16),
            ((kids, w2), F32),
        ],
        (got, dinv_par, dvar_kid),
    )


def solution(mesh):
    finer = Mesh(mesh.devices.reshape(mesh.shape["parts"], 8, 8, 2), PARTS_ROW)
    return jax.shard_map(
        device_part,
        mesh=finer,
        in_specs=(
            P(PARTS_ROW, None),
            P(PARTS_ROW, None),
            P(PARTS_ROW, None),
            P("parts", ROW, None),
            P("parts", ROW, None),
            P("parts", None),
            P("parts", None),
            P("parts", None, None),
            P("parts", None, None),
        ),
        out_specs=(
            P(PARTS_ROW, None),
            P(PARTS_ROW, None),
            P("parts", ROW, None),
            P("parts", ROW, None),
            P("parts", None),
        ),
        check_vma=False,
    )
```

```python
import jax
import jax.numpy as jnp
from jax import lax
from jax.experimental import pallas as pl
from jax.experimental.pallas import tpu as pltpu
from jax.sharding import Mesh
from jax.sharding import PartitionSpec as P

BLK = 256
LANES = 128
HALF = LANES // 2
ROW = ("y", "x", "c")
PARTS_ROW = ("parts", "y", "x", "c")
XC = ("x", "c")
F32 = jnp.float32
BF16 = jnp.bfloat16
VMEM = pl.BlockSpec(memory_space=pltpu.VMEM)
SMEM = pl.BlockSpec(memory_space=pltpu.SMEM)


def exchanged(x, axes):
    return lax.all_to_all(x, axes, split_axis=0, concat_axis=0, tiled=True)


def swapped(x, axis, bit):
    return lax.ppermute(x, axis, [(i, i ^ bit) for i in range(lax.axis_size(axis))])


def dot(a, b):
    return jnp.dot(a, b, preferred_element_type=F32)


def dot_t(a, b):
    return lax.dot_general(a, b, (((0,), (0,)), ((), ())), preferred_element_type=F32)


def turned(x):
    return pltpu.roll(x, HALF, x.ndim - 1)


def low_high(low, high):
    lane = lax.broadcasted_iota(jnp.int32, low.shape, low.ndim - 1)
    return jnp.where(lane < HALF, low, high)


def split3(v):
    parts = []
    for _ in range(3):
        top = v.astype(BF16).astype(F32)
        parts.append(top)
        v = v - top
    return parts


def call(kernel, outs, args, specs=None, scratch=()):
    return pl.pallas_call(
        kernel,
        out_shape=tuple(jax.ShapeDtypeStruct(s, d) for s, d in outs),
        in_specs=specs or [VMEM] * len(args),
        out_specs=tuple(VMEM for _ in outs),
        scratch_shapes=scratch,
        compiler_params=pltpu.CompilerParams(vmem_limit_bytes=48 * 2**20),
    )(*args)


def fetched(sources, scratch, done):
    pairs = enumerate(zip(sources, scratch))
    copies = [pltpu.make_async_copy(a, b, done.at[i]) for i, (a, b) in pairs]
    for copy in copies:
        copy.start()
    for copy in copies:
        copy.wait()


def lane_of(mask, at):
    lane = lax.broadcasted_iota(jnp.int32, mask.shape, 1)
    return jnp.sum(jnp.where(lane == at, mask, 0).astype(F32), axis=1, keepdims=True)


def pack_kernel(*refs):
    sources, (slots, par_rows, rows), scratch, done = refs[:8], refs[8:11], refs[11:19], refs[19]
    fetched(sources, scratch, done)
    sigma, par, dinv, kid_top, kid_par, mask_par, mask_kid_top, mask_kid_par = scratch
    rt, w1 = par.shape
    kids, rp = kid_par.shape[:2]
    nj = slots.shape[0]
    position = lax.axis_index(ROW)
    block_top = lax.div(position * rt, BLK)
    block_par = lax.div(position * rp, BLK)
    keep = lane_of(mask_par[...], block_top)
    packed = []
    for m in range(w1 // LANES):
        at = slice(m * LANES, (m + 1) * LANES)
        block = m * LANES // BLK
        piece = par[:, at].astype(F32) * keep[block : block + 1]
        par_rows[:, at] = piece.astype(BF16)
        top, low = piece[:rp], piece[rp:]
        packed.append(low_high(top, turned(low)))
        packed.append(low_high(turned(top), low))
    per_kid = nj // kids
    for k in range(kids):
        keep_top = lane_of(mask_kid_top[k], block_top)
        keep_par = mask_kid_par[k, pl.ds(block_par, 1), :].astype(F32)
        for m in range(per_kid):
            j = k * per_kid + m
            at = slice(m * LANES, (m + 1) * LANES)
            block = m * LANES // BLK
            piece = kid_par[k, :, at].astype(F32) * keep_par[:, block : block + 1]
            slots[j, 0 : 2 * rp, :] = jnp.concatenate([piece, packed[j]], axis=0).astype(BF16)
            piece = kid_top[k, :, at].astype(F32) * keep_top[block : block + 1]
            slots[j, 2 * rp : 2 * rp + rt, :] = piece.astype(BF16)
    rows[0:rt, :] = sigma[:, 0:w1]
    rows[rt : 2 * rt, :] = sigma[:, w1 : 2 * w1]
    rows[2 * rt : 2 * rt + rp, :] = dinv[...].astype(BF16)


def copy_kernel(*refs):
    sources, results, scratch, done = refs[:2], refs[2:4], refs[4:6], refs[6]
    fetched(sources, scratch, done)
    for result, value in zip(results, scratch):
        result[...] = value[...]


def stack_kernel(own, other, stacked):
    stacked[0] = own[...]
    stacked[1] = other[...]


def join_kernel(own, other, joined):
    count = own.shape[0]
    joined[0:count] = own[...]
    joined[count : 2 * count] = other[...]


def repeat_kernel(cols, send):
    rows = send.shape[2]
    for y in range(send.shape[0]):
        send[y] = cols[:, 0:rows, :]


def kid_par_columns(tall):
    ny, nj, rp, _ = tall.shape
    return tall[...].astype(F32).reshape(ny * nj * rp, LANES).astype(BF16)


def chunk_place(x_me, c_me, bits):
    b1, b2, b4, bc = bits
    return 2 * jnp.bitwise_xor(x_me, b1 + 2 * b2 + 4 * b4) + jnp.bitwise_xor(c_me, bc)


def step_kernel(rt, rp, cols, tall, par_own, par_other, rounded, step):
    x_me, c_me = lax.axis_index("x"), lax.axis_index("c")
    kid_par_j = kid_par_columns(tall)
    for bc, par in enumerate((par_own, par_other)):
        count, _, w1 = par.shape
        product = dot(par[...].reshape(count * rt, w1), kid_par_j)
        for k in range(count):
            at = chunk_place(x_me, c_me, (k // 4, (k // 2) % 2, k % 2, bc))
            total = cols[at, 2 * rp : 2 * rp + rt, :].astype(F32) + product[k * rt : (k + 1) * rt]
            step[at] = total
            rounded[at, 0:rt, :] = total.astype(BF16)
            rounded[at, rt : rt + rp, :] = cols[at, rp : 2 * rp, :]


def main_kernel(rt, rp, near, far, par_own, par_other, tall, cols, step, *refs):
    steps, (slots, part, db, step_j, par_j) = refs[:-5], refs[-5:]
    for k, rows in enumerate(steps):
        y = jnp.bitwise_xor(lax.axis_index("y"), k)
        step_j[y] = rows[:, 0:rt, :]
        par_j[y] = rows[:, rt : rt + rp, :].astype(F32)
    w1 = near.shape[-1]
    ny, nj = tall.shape[:2]
    x_me, c_me = lax.axis_index("x"), lax.axis_index("c")
    kid_par_j = kid_par_columns(tall)
    par_j = par_j[...].reshape(ny * nj, 1, rp, LANES)
    par_j = jnp.concatenate([par_j, turned(par_j)], axis=1)
    par_j = par_j.reshape(ny * nj * 2 * rp, LANES).astype(BF16)
    both = jnp.concatenate([step_j[...].reshape(ny * nj * rt, LANES), par_j], axis=1)

    var = jnp.zeros((1, LANES), F32)
    xs = []
    for bc, chunks in enumerate((near, far)):
        count = chunks.shape[0]
        s0 = chunks[:, 0:rt, :].reshape(count * rt, w1)
        s1 = chunks[:, rt : 2 * rt, :].reshape(count * rt, w1)
        d = chunks[:, 2 * rt : 2 * rt + rp, :].astype(F32).reshape(count * rp, w1)
        x = dot(s0, both[:w1]) + dot(s1, both[w1:])
        db_own = dot(d.astype(BF16), kid_par_j)
        for k in range(count):
            at = chunk_place(x_me, c_me, (k // 4, (k // 2) % 2, k % 2, bc))
            piece = x[k * rt : (k + 1) * rt]
            kt = piece[:, :LANES].astype(BF16)
            part[at, 0:rt, :] = kt
            c = piece[:, LANES:]
            part[at, rt : rt + rp, :] = low_high(c[:rp], turned(c[rp:])).astype(BF16)
            db_k = db_own[k * rp : (k + 1) * rp]
            db[at] = db_k
            var = var + jnp.sum(step[at] * kt.astype(F32), axis=0, keepdims=True)
            var = var + jnp.sum(cols[at, 0:rp, :].astype(F32) * db_k, axis=0, keepdims=True)
        xs.append(x.astype(BF16))

    x = jnp.concatenate(xs, axis=0)
    p = jnp.concatenate([p[...].reshape(nj // 2 * rt, w1) for p in (par_own, par_other)], axis=0)
    for y in range(ny):
        partial = dot_t(p[:, y * LANES : (y + 1) * LANES], x)
        rows = partial.shape[0]
        slots[y, 0:rows, :] = partial[:, :LANES].astype(BF16)
        q = partial[:, LANES:]
        q = low_high(q[: rows // 2], turned(q[rows // 2 :]))
        slots[y, rows : rows + rows // 2, :] = q.astype(BF16)
    var_rows = jnp.concatenate(split3(var) + [jnp.zeros((5, LANES), F32)], axis=0).astype(BF16)
    for y in range(ny):
        slots[y, rows + rows // 2 : rows + rows // 2 + 8, :] = var_rows


def sum_kernel(rt, rp, received, db, part, out):
    ny = received.shape[0]
    nj = out.shape[0]
    rows = nj * rp
    total = received[0].astype(F32)
    for y in range(1, ny):
        total = total + received[y].astype(F32)
    q = total[rows : rows + rows // 2]
    q = jnp.concatenate([q, turned(q)], axis=0)
    first = rows + rows // 2
    var = total[first : first + 1] + total[first + 1 : first + 2] + total[first + 2 : first + 3]
    var_rows = []
    for top in split3(var):
        var_rows += [turned(top), top]
    var_rows = jnp.concatenate(var_rows + [jnp.zeros((2, LANES), F32)], axis=0)
    for j in range(nj):
        at = slice(j * rp, (j + 1) * rp)
        out[j, 0 : rt + rp, :] = part[j]
        kp = total[at] + db[j]
        out[j, rt + rp : rt + 3 * rp, :] = jnp.concatenate(
            [kp, low_high(q[at], var_rows)], axis=0
        ).astype(BF16)


def final_kernel(rt, rp, got, dinv, dvar, cross_par, sigma_par, kid_top, kid_par, variance):
    nj = got.shape[0]
    kids = dvar.shape[0]
    per_kid = nj // kids
    for j in range(nj):
        k, m = divmod(j, per_kid)
        at = slice(m * LANES, (m + 1) * LANES)
        kid_top[k, :, at] = got[j, 0:rt, :]
        kid_par[k, :, at] = got[j, rt + rp : rt + 2 * rp, :]
        v = got[j, rt + 2 * rp : rt + 3 * rp, :].astype(F32)
        low = v[0:1] + v[2:3] + v[4:5]
        high = v[1:2] + v[3:4] + v[5:6]
        variance[k : k + 1, at] = dvar[k : k + 1, at] + low_high(turned(low), high)
    for m in range(nj // 2):
        at = slice(m * LANES, (m + 1) * LANES)
        a = got[2 * m, rt : rt + rp, :].astype(F32)
        b = got[2 * m + 1, rt : rt + rp, :].astype(F32)
        cross_par[:, at] = jnp.concatenate(
            [low_high(a, turned(b)), low_high(turned(a), b)], axis=0
        ).astype(BF16)
        a = got[2 * m, rt + 2 * rp : rt + 3 * rp, :].astype(F32)
        b = got[2 * m + 1, rt + 2 * rp : rt + 3 * rp, :].astype(F32)
        sigma_par[:, at] = (dinv[:, at] + low_high(a, turned(b))).astype(BF16)


def device_part(
    sigma_top,
    panel_par,
    dinv_par,
    panel_kid_top,
    panel_kid_par,
    dvar_kid,
    mask_par,
    mask_kid_top,
    mask_kid_par,
):
    rt, wt = sigma_top.shape
    rp, w1 = dinv_par.shape
    kids, _, w2 = panel_kid_top.shape
    ny = lax.axis_size("y")
    nx = lax.axis_size("x")
    nj = lax.axis_size(XC)
    assert kids * w2 == nj * LANES and w1 == nj * HALF and wt == 2 * w1
    assert nx == 8 and rt == 2 * rp and nj * rp == LANES and ny * LANES == w1

    def fetching(kernel, outs, arrays):
        return call(
            kernel,
            outs,
            tuple(pltpu.with_memory_space_constraint(a, pltpu.HBM) for a in arrays),
            [pl.BlockSpec(memory_space=pltpu.HBM)] * len(arrays),
            [pltpu.VMEM(a.shape, a.dtype) for a in arrays]
            + [pltpu.SemaphoreType.DMA((len(arrays),))],
        )

    masks = (mask_par.T, mask_kid_top.transpose(0, 2, 1), mask_kid_par)
    slots, par_rows, rows = fetching(
        pack_kernel,
        [
            ((nj, 2 * rp + rt, LANES), BF16),
            ((rt, w1), BF16),
            ((2 * rt + rp, w1), BF16),
        ],
        (sigma_top, panel_par, dinv_par, panel_kid_top, panel_kid_par, *masks),
    )
    cols = exchanged(slots, XC)
    par_far = swapped(par_rows, "x", 4)
    far_rows = swapped(rows, "x", 4)
    pair = (dvar_kid, dinv_par)
    dvar_kid, dinv_par = fetching(copy_kernel, [(a.shape, F32) for a in pair], pair)
    (tall_send,) = call(repeat_kernel, [((ny, nj, rp, LANES), BF16)], (cols,))
    par_rows = jnp.stack([par_rows, par_far])
    par_far = swapped(par_rows, "x", 2)
    tall = exchanged(tall_send, "y")
    (rows,) = call(stack_kernel, [((2, 2 * rt + rp, w1), BF16)], (rows, far_rows))
    (par_rows,) = call(join_kernel, [((4, rt, w1), BF16)], (par_rows, par_far))
    par_own = jnp.concatenate([par_rows, swapped(par_rows, "x", 1)])
    par_other = swapped(par_own, "c", 1)
    rows_2 = swapped(rows, "x", 2)
    (rows,) = call(join_kernel, [((4, 2 * rt + rp, w1), BF16)], (rows, rows_2))
    near = jnp.concatenate([rows, swapped(rows, "x", 1)])
    far = swapped(near, "c", 1)

    def sized(kernel):
        return lambda *refs: kernel(rt, rp, *refs)

    rounded, step = call(
        sized(step_kernel),
        [((nj, rt + rp, LANES), BF16), ((nj, rt, LANES), F32)],
        (cols, tall, par_own, par_other),
    )
    steps = [rounded]
    for k in range(1, ny):
        steps.append(swapped(rounded, "y", k))
    rows4 = nj * rp + nj * rp // 2 + 8
    slots4, part, db = call(
        sized(main_kernel),
        [((ny, rows4, LANES), BF16), ((nj, rt + rp, LANES), BF16), ((nj, rp, LANES), F32)],
        (near, far, par_own, par_other, tall, cols, step, *steps),
        scratch=[
            pltpu.VMEM((ny, nj, rt, LANES), BF16),
            pltpu.VMEM((ny, nj, rp, LANES), F32),
        ],
    )
    received = exchanged(slots4, "y")
    (out,) = call(
        sized(sum_kernel), [((nj, rt + 3 * rp, LANES), BF16)], (received, db, part)
    )
    got = exchanged(out, XC)
    return call(
        sized(final_kernel),
        [
            ((rt, w1), BF16),
            ((rp, w1), BF16),
            ((kids, rt, w2), BF16),
            ((kids, rp, w2), BF16),
            ((kids, w2), F32),
        ],
        (got, dinv_par, dvar_kid),
    )


def solution(mesh):
    finer = Mesh(mesh.devices.reshape(mesh.shape["parts"], 8, 8, 2), PARTS_ROW)
    return jax.shard_map(
        device_part,
        mesh=finer,
        in_specs=(
            P(PARTS_ROW, None),
            P(PARTS_ROW, None),
            P(PARTS_ROW, None),
            P("parts", ROW, None),
            P("parts", ROW, None),
            P("parts", None),
            P("parts", None),
            P("parts", None, None),
            P("parts", None, None),
        ),
        out_specs=(
            P(PARTS_ROW, None),
            P(PARTS_ROW, None),
            P("parts", ROW, None),
            P("parts", ROW, None),
            P("parts", None),
        ),
        check_vma=False,
    )
```

```python
import jax
import jax.numpy as jnp
from jax import lax
from jax.experimental import pallas as pl
from jax.experimental.pallas import tpu as pltpu
from jax.sharding import Mesh
from jax.sharding import PartitionSpec as P

BLK = 256
LANES = 128
HALF = LANES // 2
ROW = ("y", "x", "c")
PARTS_ROW = ("parts", "y", "x", "c")
XC = ("x", "c")
F32 = jnp.float32
BF16 = jnp.bfloat16
VMEM = pl.BlockSpec(memory_space=pltpu.VMEM)
SMEM = pl.BlockSpec(memory_space=pltpu.SMEM)


def exchanged(x, axes):
    return lax.all_to_all(x, axes, split_axis=0, concat_axis=0, tiled=True)


def swapped(x, axis, bit):
    return lax.ppermute(x, axis, [(i, i ^ bit) for i in range(lax.axis_size(axis))])


def dot(a, b):
    return jnp.dot(a, b, preferred_element_type=F32)


def dot_t(a, b):
    return lax.dot_general(a, b, (((0,), (0,)), ((), ())), preferred_element_type=F32)


def turned(x):
    return pltpu.roll(x, HALF, x.ndim - 1)


def low_high(low, high):
    lane = lax.broadcasted_iota(jnp.int32, low.shape, low.ndim - 1)
    return jnp.where(lane < HALF, low, high)


def split3(v):
    parts = []
    for _ in range(3):
        top = v.astype(BF16).astype(F32)
        parts.append(top)
        v = v - top
    return parts


def call(kernel, outs, args, specs=None, scratch=()):
    return pl.pallas_call(
        kernel,
        out_shape=tuple(jax.ShapeDtypeStruct(s, d) for s, d in outs),
        in_specs=specs or [VMEM] * len(args),
        out_specs=tuple(VMEM for _ in outs),
        scratch_shapes=scratch,
        compiler_params=pltpu.CompilerParams(vmem_limit_bytes=48 * 2**20),
    )(*args)


def fetched(sources, scratch, done):
    pairs = enumerate(zip(sources, scratch))
    copies = [pltpu.make_async_copy(a, b, done.at[i]) for i, (a, b) in pairs]
    for copy in copies:
        copy.start()
    for copy in copies:
        copy.wait()


def lane_of(mask, at):
    lane = lax.broadcasted_iota(jnp.int32, mask.shape, 1)
    return jnp.sum(jnp.where(lane == at, mask, 0).astype(F32), axis=1, keepdims=True)


def pack_kernel(*refs):
    sources, (slots, par_rows, rows), scratch, done = refs[:8], refs[8:11], refs[11:19], refs[19]
    fetched(sources, scratch, done)
    sigma, par, dinv, kid_top, kid_par, mask_par, mask_kid_top, mask_kid_par = scratch
    rt, w1 = par.shape
    kids, rp = kid_par.shape[:2]
    nj = slots.shape[0]
    position = lax.axis_index(ROW)
    block_top = lax.div(position * rt, BLK)
    block_par = lax.div(position * rp, BLK)
    keep = lane_of(mask_par[...], block_top)
    packed = []
    for m in range(w1 // LANES):
        at = slice(m * LANES, (m + 1) * LANES)
        block = m * LANES // BLK
        piece = par[:, at].astype(F32) * keep[block : block + 1]
        par_rows[:, at] = piece.astype(BF16)
        top, low = piece[:rp], piece[rp:]
        packed.append(low_high(top, turned(low)))
        packed.append(low_high(turned(top), low))
    per_kid = nj // kids
    for k in range(kids):
        keep_top = lane_of(mask_kid_top[k], block_top)
        keep_par = mask_kid_par[k, pl.ds(block_par, 1), :].astype(F32)
        for m in range(per_kid):
            j = k * per_kid + m
            at = slice(m * LANES, (m + 1) * LANES)
            block = m * LANES // BLK
            piece = kid_par[k, :, at].astype(F32) * keep_par[:, block : block + 1]
            slots[j, 0 : 2 * rp, :] = jnp.concatenate([piece, packed[j]], axis=0).astype(BF16)
            piece = kid_top[k, :, at].astype(F32) * keep_top[block : block + 1]
            slots[j, 2 * rp : 2 * rp + rt, :] = piece.astype(BF16)
    rows[0:rt, :] = sigma[:, 0:w1]
    rows[rt : 2 * rt, :] = sigma[:, w1 : 2 * w1]
    rows[2 * rt : 2 * rt + rp, :] = dinv[...].astype(BF16)


def copy_kernel(source_hbm, result, scratch, done):
    fetched((source_hbm,), (scratch,), done)
    result[...] = scratch[...]


def stack_kernel(own, other, *refs):
    refs[-1][0] = own[...]
    refs[-1][1] = other[...]


def join_kernel(own, other, joined):
    count = own.shape[0]
    joined[0:count] = own[...]
    joined[count : 2 * count] = other[...]


def repeat_kernel(cols, send):
    rows = send.shape[2]
    for y in range(send.shape[0]):
        send[y] = cols[:, 0:rows, :]


def kid_par_columns(tall):
    ny, nj, rp, _ = tall.shape
    return tall[...].astype(F32).reshape(ny * nj * rp, LANES).astype(BF16)


def chunk_place(x_me, c_me, bits):
    b1, b2, b4, bc = bits
    return 2 * jnp.bitwise_xor(x_me, b1 + 2 * b2 + 4 * b4) + jnp.bitwise_xor(c_me, bc)


def step_kernel(rt, rp, cols, tall, par_own, par_other, rounded, step):
    x_me, c_me = lax.axis_index("x"), lax.axis_index("c")
    kid_par_j = kid_par_columns(tall)
    for bc, par in enumerate((par_own, par_other)):
        count, _, w1 = par.shape
        product = dot(par[...].reshape(count * rt, w1), kid_par_j)
        for k in range(count):
            at = chunk_place(x_me, c_me, (k // 4, (k // 2) % 2, k % 2, bc))
            total = cols[at, 2 * rp : 2 * rp + rt, :].astype(F32) + product[k * rt : (k + 1) * rt]
            step[at] = total
            rounded[at, 0:rt, :] = total.astype(BF16)
            rounded[at, rt : rt + rp, :] = cols[at, rp : 2 * rp, :]


def main_kernel(rt, rp, near, far, par_own, par_other, tall, cols, step, *refs):
    steps, (slots, part, db, step_j, par_j) = refs[:-5], refs[-5:]
    for k, rows in enumerate(steps):
        y = jnp.bitwise_xor(lax.axis_index("y"), k)
        step_j[y] = rows[:, 0:rt, :]
        par_j[y] = rows[:, rt : rt + rp, :].astype(F32)
    w1 = near.shape[-1]
    ny, nj = tall.shape[:2]
    x_me, c_me = lax.axis_index("x"), lax.axis_index("c")
    kid_par_j = kid_par_columns(tall)
    par_j = par_j[...].reshape(ny * nj, 1, rp, LANES)
    par_j = jnp.concatenate([par_j, turned(par_j)], axis=1)
    par_j = par_j.reshape(ny * nj * 2 * rp, LANES).astype(BF16)
    both = jnp.concatenate([step_j[...].reshape(ny * nj * rt, LANES), par_j], axis=1)

    var = jnp.zeros((1, LANES), F32)
    xs = []
    for bc, chunks in enumerate((near, far)):
        count = chunks.shape[0]
        s0 = chunks[:, 0:rt, :].reshape(count * rt, w1)
        s1 = chunks[:, rt : 2 * rt, :].reshape(count * rt, w1)
        d = chunks[:, 2 * rt : 2 * rt + rp, :].astype(F32).reshape(count * rp, w1)
        x = dot(s0, both[:w1]) + dot(s1, both[w1:])
        db_own = dot(d.astype(BF16), kid_par_j)
        for k in range(count):
            at = chunk_place(x_me, c_me, (k // 4, (k // 2) % 2, k % 2, bc))
            piece = x[k * rt : (k + 1) * rt]
            kt = piece[:, :LANES].astype(BF16)
            part[at, 0:rt, :] = kt
            c = piece[:, LANES:]
            part[at, rt : rt + rp, :] = low_high(c[:rp], turned(c[rp:])).astype(BF16)
            db_k = db_own[k * rp : (k + 1) * rp]
            db[at] = db_k
            var = var + jnp.sum(step[at] * kt.astype(F32), axis=0, keepdims=True)
            var = var + jnp.sum(cols[at, 0:rp, :].astype(F32) * db_k, axis=0, keepdims=True)
        xs.append(x.astype(BF16))

    x = jnp.concatenate(xs, axis=0)
    p = jnp.concatenate([p[...].reshape(nj // 2 * rt, w1) for p in (par_own, par_other)], axis=0)
    for y in range(ny):
        partial = dot_t(p[:, y * LANES : (y + 1) * LANES], x)
        rows = partial.shape[0]
        slots[y, 0:rows, :] = partial[:, :LANES].astype(BF16)
        q = partial[:, LANES:]
        q = low_high(q[: rows // 2], turned(q[rows // 2 :]))
        slots[y, rows : rows + rows // 2, :] = q.astype(BF16)
    var_rows = jnp.concatenate(split3(var) + [jnp.zeros((5, LANES), F32)], axis=0).astype(BF16)
    for y in range(ny):
        slots[y, rows + rows // 2 : rows + rows // 2 + 8, :] = var_rows


def sum_kernel(rt, rp, received, db, part, out):
    ny = received.shape[0]
    nj = out.shape[0]
    rows = nj * rp
    total = received[0].astype(F32)
    for y in range(1, ny):
        total = total + received[y].astype(F32)
    q = total[rows : rows + rows // 2]
    q = jnp.concatenate([q, turned(q)], axis=0)
    first = rows + rows // 2
    var = total[first : first + 1] + total[first + 1 : first + 2] + total[first + 2 : first + 3]
    var_rows = []
    for top in split3(var):
        var_rows += [turned(top), top]
    var_rows = jnp.concatenate(var_rows + [jnp.zeros((2, LANES), F32)], axis=0)
    for j in range(nj):
        at = slice(j * rp, (j + 1) * rp)
        out[j, 0 : rt + rp, :] = part[j]
        kp = total[at] + db[j]
        out[j, rt + rp : rt + 3 * rp, :] = jnp.concatenate(
            [kp, low_high(q[at], var_rows)], axis=0
        ).astype(BF16)


def final_kernel(rt, rp, got, dinv, dvar, cross_par, sigma_par, kid_top, kid_par, variance):
    nj = got.shape[0]
    kids = dvar.shape[0]
    per_kid = nj // kids
    for j in range(nj):
        k, m = divmod(j, per_kid)
        at = slice(m * LANES, (m + 1) * LANES)
        kid_top[k, :, at] = got[j, 0:rt, :]
        kid_par[k, :, at] = got[j, rt + rp : rt + 2 * rp, :]
        v = got[j, rt + 2 * rp : rt + 3 * rp, :].astype(F32)
        low = v[0:1] + v[2:3] + v[4:5]
        high = v[1:2] + v[3:4] + v[5:6]
        variance[k : k + 1, at] = dvar[k : k + 1, at] + low_high(turned(low), high)
    for m in range(nj // 2):
        at = slice(m * LANES, (m + 1) * LANES)
        a = got[2 * m, rt : rt + rp, :].astype(F32)
        b = got[2 * m + 1, rt : rt + rp, :].astype(F32)
        cross_par[:, at] = jnp.concatenate(
            [low_high(a, turned(b)), low_high(turned(a), b)], axis=0
        ).astype(BF16)
        a = got[2 * m, rt + 2 * rp : rt + 3 * rp, :].astype(F32)
        b = got[2 * m + 1, rt + 2 * rp : rt + 3 * rp, :].astype(F32)
        sigma_par[:, at] = (dinv[:, at] + low_high(a, turned(b))).astype(BF16)


def device_part(
    sigma_top,
    panel_par,
    dinv_par,
    panel_kid_top,
    panel_kid_par,
    dvar_kid,
    mask_par,
    mask_kid_top,
    mask_kid_par,
):
    rt, wt = sigma_top.shape
    rp, w1 = dinv_par.shape
    kids, _, w2 = panel_kid_top.shape
    ny = lax.axis_size("y")
    nx = lax.axis_size("x")
    nj = lax.axis_size(XC)
    assert kids * w2 == nj * LANES and w1 == nj * HALF and wt == 2 * w1
    assert nx == 8 and rt == 2 * rp and nj * rp == LANES and ny * LANES == w1

    def fetching(kernel, outs, arrays):
        return call(
            kernel,
            outs,
            tuple(pltpu.with_memory_space_constraint(a, pltpu.HBM) for a in arrays),
            [pl.BlockSpec(memory_space=pltpu.HBM)] * len(arrays),
            [pltpu.VMEM(a.shape, a.dtype) for a in arrays]
            + [pltpu.SemaphoreType.DMA((len(arrays),))],
        )

    masks = (mask_par.T, mask_kid_top.transpose(0, 2, 1), mask_kid_par)
    slots, par_rows, rows = fetching(
        pack_kernel,
        [
            ((nj, 2 * rp + rt, LANES), BF16),
            ((rt, w1), BF16),
            ((2 * rt + rp, w1), BF16),
        ],
        (sigma_top, panel_par, dinv_par, panel_kid_top, panel_kid_par, *masks),
    )
    cols = exchanged(slots, XC)
    par_far = swapped(par_rows, "x", 4)
    far_rows = swapped(rows, "x", 4)
    (dvar_kid,) = fetching(copy_kernel, [(dvar_kid.shape, F32)], (dvar_kid,))
    (tall_send,) = call(repeat_kernel, [((ny, nj, rp, LANES), BF16)], (cols,))
    (par_rows,) = call(
        stack_kernel,
        [((2, rt, w1), BF16)],
        (par_rows, par_far, tall_send),
        [VMEM, VMEM, pl.BlockSpec(memory_space=pl.ANY)],
    )
    par_far = swapped(par_rows, "x", 2)
    tall = exchanged(tall_send, "y")
    (rows,) = call(stack_kernel, [((2, 2 * rt + rp, w1), BF16)], (rows, far_rows))
    (par_rows,) = call(join_kernel, [((4, rt, w1), BF16)], (par_rows, par_far))
    par_own = jnp.concatenate([par_rows, swapped(par_rows, "x", 1)])
    par_other = swapped(par_own, "c", 1)
    rows_2 = swapped(rows, "x", 2)
    (rows,) = call(join_kernel, [((4, 2 * rt + rp, w1), BF16)], (rows, rows_2))
    near = jnp.concatenate([rows, swapped(rows, "x", 1)])
    far = swapped(near, "c", 1)

    def sized(kernel):
        return lambda *refs: kernel(rt, rp, *refs)

    rounded, step = call(
        sized(step_kernel),
        [((nj, rt + rp, LANES), BF16), ((nj, rt, LANES), F32)],
        (cols, tall, par_own, par_other),
    )
    steps = [rounded]
    for k in range(1, ny):
        steps.append(swapped(rounded, "y", k))
    rows4 = nj * rp + nj * rp // 2 + 8
    slots4, part, db = call(
        sized(main_kernel),
        [((ny, rows4, LANES), BF16), ((nj, rt + rp, LANES), BF16), ((nj, rp, LANES), F32)],
        (near, far, par_own, par_other, tall, cols, step, *steps),
        scratch=[
            pltpu.VMEM((ny, nj, rt, LANES), BF16),
            pltpu.VMEM((ny, nj, rp, LANES), F32),
        ],
    )
    received = exchanged(slots4, "y")
    (out,) = call(
        sized(sum_kernel), [((nj, rt + 3 * rp, LANES), BF16)], (received, db, part)
    )
    got = exchanged(out, XC)
    return call(
        sized(final_kernel),
        [
            ((rt, w1), BF16),
            ((rp, w1), BF16),
            ((kids, rt, w2), BF16),
            ((kids, rp, w2), BF16),
            ((kids, w2), F32),
        ],
        (got, dinv_par, dvar_kid),
    )


def solution(mesh):
    finer = Mesh(mesh.devices.reshape(mesh.shape["parts"], 8, 8, 2), PARTS_ROW)
    return jax.shard_map(
        device_part,
        mesh=finer,
        in_specs=(
            P(PARTS_ROW, None),
            P(PARTS_ROW, None),
            P(PARTS_ROW, None),
            P("parts", ROW, None),
            P("parts", ROW, None),
            P("parts", None),
            P("parts", None),
            P("parts", None, None),
            P("parts", None, None),
        ),
        out_specs=(
            P(PARTS_ROW, None),
            P(PARTS_ROW, None),
            P("parts", ROW, None),
            P("parts", ROW, None),
            P("parts", None),
        ),
        check_vma=False,
    )
```

```python
import jax
import jax.numpy as jnp
from jax import lax
from jax.experimental import pallas as pl
from jax.experimental.pallas import tpu as pltpu
from jax.sharding import Mesh
from jax.sharding import PartitionSpec as P

BLK = 256
LANES = 128
HALF = LANES // 2
ROW = ("y", "x", "c")
PARTS_ROW = ("parts", "y", "x", "c")
XC = ("x", "c")
F32 = jnp.float32
BF16 = jnp.bfloat16
VMEM = pl.BlockSpec(memory_space=pltpu.VMEM)
SMEM = pl.BlockSpec(memory_space=pltpu.SMEM)


def exchanged(x, axes):
    return lax.all_to_all(x, axes, split_axis=0, concat_axis=0, tiled=True)


def swapped(x, axis, bit):
    return lax.ppermute(x, axis, [(i, i ^ bit) for i in range(lax.axis_size(axis))])


def dot(a, b):
    return jnp.dot(a, b, preferred_element_type=F32)


def dot_t(a, b):
    return lax.dot_general(a, b, (((0,), (0,)), ((), ())), preferred_element_type=F32)


def turned(x):
    return pltpu.roll(x, HALF, x.ndim - 1)


def low_high(low, high):
    lane = lax.broadcasted_iota(jnp.int32, low.shape, low.ndim - 1)
    return jnp.where(lane < HALF, low, high)


def split3(v):
    parts = []
    for _ in range(3):
        top = v.astype(BF16).astype(F32)
        parts.append(top)
        v = v - top
    return parts


def call(kernel, outs, args, specs=None, scratch=()):
    return pl.pallas_call(
        kernel,
        out_shape=tuple(jax.ShapeDtypeStruct(s, d) for s, d in outs),
        in_specs=specs or [VMEM] * len(args),
        out_specs=tuple(VMEM for _ in outs),
        scratch_shapes=scratch,
        compiler_params=pltpu.CompilerParams(vmem_limit_bytes=48 * 2**20),
    )(*args)


def fetched(sources, scratch, done):
    pairs = enumerate(zip(sources, scratch))
    copies = [pltpu.make_async_copy(a, b, done.at[i]) for i, (a, b) in pairs]
    for copy in copies:
        copy.start()
    for copy in copies:
        copy.wait()


def lane_of(mask, at):
    lane = lax.broadcasted_iota(jnp.int32, mask.shape, 1)
    return jnp.sum(jnp.where(lane == at, mask, 0).astype(F32), axis=1, keepdims=True)


def pack_kernel(*refs):
    sources, (slots, par_rows, rows), scratch, done = refs[:8], refs[8:11], refs[11:19], refs[19]
    fetched(sources, scratch, done)
    sigma, par, dinv, kid_top, kid_par, mask_par, mask_kid_top, mask_kid_par = scratch
    rt, w1 = par.shape
    kids, rp = kid_par.shape[:2]
    nj = slots.shape[0]
    position = lax.axis_index(ROW)
    block_top = lax.div(position * rt, BLK)
    block_par = lax.div(position * rp, BLK)
    keep = lane_of(mask_par[...], block_top)
    packed = []
    for m in range(w1 // LANES):
        at = slice(m * LANES, (m + 1) * LANES)
        block = m * LANES // BLK
        piece = par[:, at].astype(F32) * keep[block : block + 1]
        par_rows[:, at] = piece.astype(BF16)
        top, low = piece[:rp], piece[rp:]
        packed.append(low_high(top, turned(low)))
        packed.append(low_high(turned(top), low))
    per_kid = nj // kids
    for k in range(kids):
        keep_top = lane_of(mask_kid_top[k], block_top)
        keep_par = mask_kid_par[k, pl.ds(block_par, 1), :].astype(F32)
        for m in range(per_kid):
            j = k * per_kid + m
            at = slice(m * LANES, (m + 1) * LANES)
            block = m * LANES // BLK
            piece = kid_par[k, :, at].astype(F32) * keep_par[:, block : block + 1]
            slots[j, 0 : 2 * rp, :] = jnp.concatenate([piece, packed[j]], axis=0).astype(BF16)
            piece = kid_top[k, :, at].astype(F32) * keep_top[block : block + 1]
            slots[j, 2 * rp : 2 * rp + rt, :] = piece.astype(BF16)
    rows[0:rt, :] = sigma[:, 0:w1]
    rows[rt : 2 * rt, :] = sigma[:, w1 : 2 * w1]
    rows[2 * rt : 2 * rt + rp, :] = dinv[...].astype(BF16)


def copy_kernel(source_hbm, result, scratch, done):
    fetched((source_hbm,), (scratch,), done)
    result[...] = scratch[...]


def stack_kernel(own, other, *refs):
    refs[-1][0] = own[...]
    refs[-1][1] = other[...]


def join_kernel(own, other, joined):
    count = own.shape[0]
    joined[0:count] = own[...]
    joined[count : 2 * count] = other[...]


def repeat_kernel(cols, send):
    rows = send.shape[2]
    for y in range(send.shape[0]):
        send[y] = cols[:, 0:rows, :]


def kid_par_columns(tall):
    ny, nj, rp, _ = tall.shape
    return tall[...].astype(F32).reshape(ny * nj * rp, LANES).astype(BF16)


def chunk_place(x_me, c_me, bits):
    b1, b2, b4, bc = bits
    return 2 * jnp.bitwise_xor(x_me, b1 + 2 * b2 + 4 * b4) + jnp.bitwise_xor(c_me, bc)


def step_kernel(rt, rp, cols, tall, par_own, par_other, rounded, step):
    x_me, c_me = lax.axis_index("x"), lax.axis_index("c")
    kid_par_j = kid_par_columns(tall)
    for bc, par in enumerate((par_own, par_other)):
        count, _, w1 = par.shape
        product = dot(par[...].reshape(count * rt, w1), kid_par_j)
        for k in range(count):
            at = chunk_place(x_me, c_me, (k // 4, (k // 2) % 2, k % 2, bc))
            total = cols[at, 2 * rp : 2 * rp + rt, :].astype(F32) + product[k * rt : (k + 1) * rt]
            step[at] = total
            rounded[at, 0:rt, :] = total.astype(BF16)
            rounded[at, rt : rt + rp, :] = cols[at, rp : 2 * rp, :]


def main_kernel(rt, rp, near, far, par_own, par_other, tall, cols, step, *refs):
    steps, slots, (part, db, step_j, par_j) = refs[:8], refs[8:16], refs[16:]
    for k, rows in enumerate(steps):
        y = jnp.bitwise_xor(lax.axis_index("y"), k)
        step_j[y] = rows[:, 0:rt, :]
        par_j[y] = rows[:, rt : rt + rp, :].astype(F32)
    w1 = near.shape[-1]
    ny, nj = tall.shape[:2]
    x_me, c_me = lax.axis_index("x"), lax.axis_index("c")
    kid_par_j = kid_par_columns(tall)
    par_j = par_j[...].reshape(ny * nj, 1, rp, LANES)
    par_j = jnp.concatenate([par_j, turned(par_j)], axis=1)
    par_j = par_j.reshape(ny * nj * 2 * rp, LANES).astype(BF16)
    both = jnp.concatenate([step_j[...].reshape(ny * nj * rt, LANES), par_j], axis=1)

    var = jnp.zeros((1, LANES), F32)
    xs = []
    for bc, chunks in enumerate((near, far)):
        count = chunks.shape[0]
        s0 = chunks[:, 0:rt, :].reshape(count * rt, w1)
        s1 = chunks[:, rt : 2 * rt, :].reshape(count * rt, w1)
        d = chunks[:, 2 * rt : 2 * rt + rp, :].astype(F32).reshape(count * rp, w1)
        x = dot(s0, both[:w1]) + dot(s1, both[w1:])
        db_own = dot(d.astype(BF16), kid_par_j)
        for k in range(count):
            at = chunk_place(x_me, c_me, (k // 4, (k // 2) % 2, k % 2, bc))
            piece = x[k * rt : (k + 1) * rt]
            kt = piece[:, :LANES].astype(BF16)
            part[at, 0:rt, :] = kt
            c = piece[:, LANES:]
            part[at, rt : rt + rp, :] = low_high(c[:rp], turned(c[rp:])).astype(BF16)
            db_k = db_own[k * rp : (k + 1) * rp]
            db[at] = db_k
            var = var + jnp.sum(step[at] * kt.astype(F32), axis=0, keepdims=True)
            var = var + jnp.sum(cols[at, 0:rp, :].astype(F32) * db_k, axis=0, keepdims=True)
        xs.append(x.astype(BF16))

    x = jnp.concatenate(xs, axis=0)
    var_rows = jnp.concatenate(split3(var) + [jnp.zeros((5, LANES), F32)], axis=0)
    for k, slot in enumerate(slots):
        y = jnp.bitwise_xor(lax.axis_index("y"), k)
        at = pl.ds(pl.multiple_of(y * LANES, LANES), LANES)
        p = [p[:, :, at].reshape(nj // 2 * rt, LANES) for p in (par_own, par_other)]
        partial = dot_t(jnp.concatenate(p, axis=0), x)
        rows = partial.shape[0]
        slot[0:rows, :] = partial[:, :LANES].astype(BF16)
        q = partial[:, LANES:]
        q = low_high(q[: rows // 2], turned(q[rows // 2 :]))
        slot[rows : rows + rows // 2 + 8, :] = jnp.concatenate([q, var_rows], axis=0).astype(BF16)


def sum_kernel(rt, rp, *refs):
    received, (db, part, out) = refs[:-3], refs[-3:]
    nj = out.shape[0]
    rows = nj * rp
    total = received[0][...].astype(F32)
    for one in received[1:]:
        total = total + one[...].astype(F32)
    q = total[rows : rows + rows // 2]
    q = jnp.concatenate([q, turned(q)], axis=0)
    first = rows + rows // 2
    var = total[first : first + 1] + total[first + 1 : first + 2] + total[first + 2 : first + 3]
    var_rows = []
    for top in split3(var):
        var_rows += [turned(top), top]
    var_rows = jnp.concatenate(var_rows + [jnp.zeros((2, LANES), F32)], axis=0)
    for j in range(nj):
        at = slice(j * rp, (j + 1) * rp)
        out[j, 0 : rt + rp, :] = part[j]
        kp = total[at] + db[j]
        out[j, rt + rp : rt + 3 * rp, :] = jnp.concatenate(
            [kp, low_high(q[at], var_rows)], axis=0
        ).astype(BF16)


def final_kernel(rt, rp, got, dinv, dvar, cross_par, sigma_par, kid_top, kid_par, variance):
    nj = got.shape[0]
    kids = dvar.shape[0]
    per_kid = nj // kids
    for j in range(nj):
        k, m = divmod(j, per_kid)
        at = slice(m * LANES, (m + 1) * LANES)
        kid_top[k, :, at] = got[j, 0:rt, :]
        kid_par[k, :, at] = got[j, rt + rp : rt + 2 * rp, :]
        v = got[j, rt + 2 * rp : rt + 3 * rp, :].astype(F32)
        low = v[0:1] + v[2:3] + v[4:5]
        high = v[1:2] + v[3:4] + v[5:6]
        variance[k : k + 1, at] = dvar[k : k + 1, at] + low_high(turned(low), high)
    for m in range(nj // 2):
        at = slice(m * LANES, (m + 1) * LANES)
        a = got[2 * m, rt : rt + rp, :].astype(F32)
        b = got[2 * m + 1, rt : rt + rp, :].astype(F32)
        cross_par[:, at] = jnp.concatenate(
            [low_high(a, turned(b)), low_high(turned(a), b)], axis=0
        ).astype(BF16)
        a = got[2 * m, rt + 2 * rp : rt + 3 * rp, :].astype(F32)
        b = got[2 * m + 1, rt + 2 * rp : rt + 3 * rp, :].astype(F32)
        sigma_par[:, at] = (dinv[:, at] + low_high(a, turned(b))).astype(BF16)


def device_part(
    sigma_top,
    panel_par,
    dinv_par,
    panel_kid_top,
    panel_kid_par,
    dvar_kid,
    mask_par,
    mask_kid_top,
    mask_kid_par,
):
    rt, wt = sigma_top.shape
    rp, w1 = dinv_par.shape
    kids, _, w2 = panel_kid_top.shape
    ny = lax.axis_size("y")
    nx = lax.axis_size("x")
    nj = lax.axis_size(XC)
    assert kids * w2 == nj * LANES and w1 == nj * HALF and wt == 2 * w1
    assert nx == 8 and rt == 2 * rp and nj * rp == LANES and ny * LANES == w1

    def fetching(kernel, outs, arrays):
        return call(
            kernel,
            outs,
            tuple(pltpu.with_memory_space_constraint(a, pltpu.HBM) for a in arrays),
            [pl.BlockSpec(memory_space=pltpu.HBM)] * len(arrays),
            [pltpu.VMEM(a.shape, a.dtype) for a in arrays]
            + [pltpu.SemaphoreType.DMA((len(arrays),))],
        )

    masks = (mask_par.T, mask_kid_top.transpose(0, 2, 1), mask_kid_par)
    slots, par_rows, rows = fetching(
        pack_kernel,
        [
            ((nj, 2 * rp + rt, LANES), BF16),
            ((rt, w1), BF16),
            ((2 * rt + rp, w1), BF16),
        ],
        (sigma_top, panel_par, dinv_par, panel_kid_top, panel_kid_par, *masks),
    )
    cols = exchanged(slots, XC)
    par_far = swapped(par_rows, "x", 4)
    far_rows = swapped(rows, "x", 4)
    (dvar_kid,) = fetching(copy_kernel, [(dvar_kid.shape, F32)], (dvar_kid,))
    (tall_send,) = call(repeat_kernel, [((ny, nj, rp, LANES), BF16)], (cols,))
    (par_rows,) = call(
        stack_kernel,
        [((2, rt, w1), BF16)],
        (par_rows, par_far, tall_send),
        [VMEM, VMEM, pl.BlockSpec(memory_space=pl.ANY)],
    )
    par_far = swapped(par_rows, "x", 2)
    tall = exchanged(tall_send, "y")
    (rows,) = call(stack_kernel, [((2, 2 * rt + rp, w1), BF16)], (rows, far_rows))
    (par_rows,) = call(join_kernel, [((4, rt, w1), BF16)], (par_rows, par_far))
    par_own = jnp.concatenate([par_rows, swapped(par_rows, "x", 1)])
    par_other = swapped(par_own, "c", 1)
    rows_2 = swapped(rows, "x", 2)
    (rows,) = call(join_kernel, [((4, 2 * rt + rp, w1), BF16)], (rows, rows_2))
    near = jnp.concatenate([rows, swapped(rows, "x", 1)])
    far = swapped(near, "c", 1)

    def sized(kernel):
        return lambda *refs: kernel(rt, rp, *refs)

    rounded, step = call(
        sized(step_kernel),
        [((nj, rt + rp, LANES), BF16), ((nj, rt, LANES), F32)],
        (cols, tall, par_own, par_other),
    )
    steps = [rounded]
    for k in range(1, ny):
        steps.append(swapped(rounded, "y", k))
    rows4 = nj * rp + nj * rp // 2 + 8
    *partials, part, db = call(
        sized(main_kernel),
        [((rows4, LANES), BF16)] * ny
        + [((nj, rt + rp, LANES), BF16), ((nj, rp, LANES), F32)],
        (near, far, par_own, par_other, tall, cols, step, *steps),
        scratch=[
            pltpu.VMEM((ny, nj, rt, LANES), BF16),
            pltpu.VMEM((ny, nj, rp, LANES), F32),
        ],
    )
    for k in range(1, ny):
        partials[k] = swapped(partials[k], "y", k)
    (out,) = call(sized(sum_kernel), [((nj, rt + 3 * rp, LANES), BF16)], (*partials, db, part))
    got = exchanged(out, XC)
    return call(
        sized(final_kernel),
        [
            ((rt, w1), BF16),
            ((rp, w1), BF16),
            ((kids, rt, w2), BF16),
            ((kids, rp, w2), BF16),
            ((kids, w2), F32),
        ],
        (got, dinv_par, dvar_kid),
    )


def solution(mesh):
    finer = Mesh(mesh.devices.reshape(mesh.shape["parts"], 8, 8, 2), PARTS_ROW)
    return jax.shard_map(
        device_part,
        mesh=finer,
        in_specs=(
            P(PARTS_ROW, None),
            P(PARTS_ROW, None),
            P(PARTS_ROW, None),
            P("parts", ROW, None),
            P("parts", ROW, None),
            P("parts", None),
            P("parts", None),
            P("parts", None, None),
            P("parts", None, None),
        ),
        out_specs=(
            P(PARTS_ROW, None),
            P(PARTS_ROW, None),
            P("parts", ROW, None),
            P("parts", ROW, None),
            P("parts", None),
        ),
        check_vma=False,
    )
```

```python
import jax
import jax.numpy as jnp
from jax import lax
from jax.experimental import pallas as pl
from jax.experimental.pallas import tpu as pltpu
from jax.sharding import Mesh
from jax.sharding import PartitionSpec as P

BLK = 256
LANES = 128
HALF = LANES // 2
ROW = ("y", "x", "c")
PARTS_ROW = ("parts", "y", "x", "c")
XC = ("x", "c")
F32 = jnp.float32
BF16 = jnp.bfloat16
VMEM = pl.BlockSpec(memory_space=pltpu.VMEM)
SMEM = pl.BlockSpec(memory_space=pltpu.SMEM)


def exchanged(x, axes):
    return lax.all_to_all(x, axes, split_axis=0, concat_axis=0, tiled=True)


def swapped(x, axis, bit):
    return lax.ppermute(x, axis, [(i, i ^ bit) for i in range(lax.axis_size(axis))])


def dot(a, b):
    return jnp.dot(a, b, preferred_element_type=F32)


def dot_t(a, b):
    return lax.dot_general(a, b, (((0,), (0,)), ((), ())), preferred_element_type=F32)


def turned(x):
    return pltpu.roll(x, HALF, x.ndim - 1)


def low_high(low, high):
    lane = lax.broadcasted_iota(jnp.int32, low.shape, low.ndim - 1)
    return jnp.where(lane < HALF, low, high)


def split3(v):
    parts = []
    for _ in range(3):
        top = v.astype(BF16).astype(F32)
        parts.append(top)
        v = v - top
    return parts


def call(kernel, outs, args, specs=None, scratch=()):
    return pl.pallas_call(
        kernel,
        out_shape=tuple(jax.ShapeDtypeStruct(s, d) for s, d in outs),
        in_specs=specs or [VMEM] * len(args),
        out_specs=tuple(VMEM for _ in outs),
        scratch_shapes=scratch,
        compiler_params=pltpu.CompilerParams(vmem_limit_bytes=48 * 2**20),
    )(*args)


def fetched(sources, scratch, done):
    pairs = enumerate(zip(sources, scratch))
    copies = [pltpu.make_async_copy(a, b, done.at[i]) for i, (a, b) in pairs]
    for copy in copies:
        copy.start()
    for copy in copies:
        copy.wait()


def lane_of(mask, at):
    lane = lax.broadcasted_iota(jnp.int32, mask.shape, 1)
    return jnp.sum(jnp.where(lane == at, mask, 0).astype(F32), axis=1, keepdims=True)


def pack_kernel(*refs):
    sources, (slots, par_rows, rows), scratch, done = refs[:8], refs[8:11], refs[11:19], refs[19]
    fetched(sources, scratch, done)
    sigma, par, dinv, kid_top, kid_par, mask_par, mask_kid_top, mask_kid_par = scratch
    rt, w1 = par.shape
    kids, rp = kid_par.shape[:2]
    nj = slots.shape[0]
    position = lax.axis_index(ROW)
    block_top = lax.div(position * rt, BLK)
    block_par = lax.div(position * rp, BLK)
    keep = lane_of(mask_par[...], block_top)
    packed = []
    for m in range(w1 // LANES):
        at = slice(m * LANES, (m + 1) * LANES)
        block = m * LANES // BLK
        piece = par[:, at].astype(F32) * keep[block : block + 1]
        par_rows[:, at] = piece.astype(BF16)
        top, low = piece[:rp], piece[rp:]
        packed.append(low_high(top, turned(low)))
        packed.append(low_high(turned(top), low))
    per_kid = nj // kids
    for k in range(kids):
        keep_top = lane_of(mask_kid_top[k], block_top)
        keep_par = mask_kid_par[k, pl.ds(block_par, 1), :].astype(F32)
        for m in range(per_kid):
            j = k * per_kid + m
            at = slice(m * LANES, (m + 1) * LANES)
            block = m * LANES // BLK
            piece = kid_par[k, :, at].astype(F32) * keep_par[:, block : block + 1]
            slots[j, 0 : 2 * rp, :] = jnp.concatenate([piece, packed[j]], axis=0).astype(BF16)
            piece = kid_top[k, :, at].astype(F32) * keep_top[block : block + 1]
            slots[j, 2 * rp : 2 * rp + rt, :] = piece.astype(BF16)
    rows[0:rt, :] = sigma[:, 0:w1]
    rows[rt : 2 * rt, :] = sigma[:, w1 : 2 * w1]
    rows[2 * rt : 2 * rt + rp, :] = dinv[...].astype(BF16)


def copy_kernel(source, result):
    result[...] = source[...]


def stack_kernel(own, other, *refs):
    refs[-1][0] = own[...]
    refs[-1][1] = other[...]


def join_kernel(own, other, joined):
    count = own.shape[0]
    joined[0:count] = own[...]
    joined[count : 2 * count] = other[...]


def repeat_kernel(cols, send):
    rows = send.shape[2]
    for y in range(send.shape[0]):
        send[y] = cols[:, 0:rows, :]


def kid_par_columns(tall):
    ny, nj, rp, _ = tall.shape
    return tall[...].astype(F32).reshape(ny * nj * rp, LANES).astype(BF16)


def chunk_place(x_me, c_me, bits):
    b1, b2, b4, bc = bits
    return 2 * jnp.bitwise_xor(x_me, b1 + 2 * b2 + 4 * b4) + jnp.bitwise_xor(c_me, bc)


def step_kernel(rt, rp, cols, tall, par_own, par_other, rounded, step):
    x_me, c_me = lax.axis_index("x"), lax.axis_index("c")
    kid_par_j = kid_par_columns(tall)
    for bc, par in enumerate((par_own, par_other)):
        count, _, w1 = par.shape
        product = dot(par[...].reshape(count * rt, w1), kid_par_j)
        for k in range(count):
            at = chunk_place(x_me, c_me, (k // 4, (k // 2) % 2, k % 2, bc))
            total = cols[at, 2 * rp : 2 * rp + rt, :].astype(F32) + product[k * rt : (k + 1) * rt]
            step[at] = total
            rounded[at, 0:rt, :] = total.astype(BF16)
            rounded[at, rt : rt + rp, :] = cols[at, rp : 2 * rp, :]


def main_kernel(rt, rp, near, far, par_own, par_other, tall, cols, step, *refs):
    steps, slots, (part, db, step_j, par_j) = refs[:8], refs[8:16], refs[16:]
    for k, rows in enumerate(steps):
        y = jnp.bitwise_xor(lax.axis_index("y"), k)
        step_j[y] = rows[:, 0:rt, :]
        par_j[y] = rows[:, rt : rt + rp, :].astype(F32)
    w1 = near.shape[-1]
    ny, nj = tall.shape[:2]
    x_me, c_me = lax.axis_index("x"), lax.axis_index("c")
    kid_par_j = kid_par_columns(tall)
    par_j = par_j[...].reshape(ny * nj, 1, rp, LANES)
    par_j = jnp.concatenate([par_j, turned(par_j)], axis=1)
    par_j = par_j.reshape(ny * nj * 2 * rp, LANES).astype(BF16)
    both = jnp.concatenate([step_j[...].reshape(ny * nj * rt, LANES), par_j], axis=1)

    var = jnp.zeros((1, LANES), F32)
    xs = []
    for bc, chunks in enumerate((near, far)):
        count = chunks.shape[0]
        s0 = chunks[:, 0:rt, :].reshape(count * rt, w1)
        s1 = chunks[:, rt : 2 * rt, :].reshape(count * rt, w1)
        d = chunks[:, 2 * rt : 2 * rt + rp, :].astype(F32).reshape(count * rp, w1)
        x = dot(s0, both[:w1]) + dot(s1, both[w1:])
        db_own = dot(d.astype(BF16), kid_par_j)
        for k in range(count):
            at = chunk_place(x_me, c_me, (k // 4, (k // 2) % 2, k % 2, bc))
            piece = x[k * rt : (k + 1) * rt]
            kt = piece[:, :LANES].astype(BF16)
            part[at, 0:rt, :] = kt
            c = piece[:, LANES:]
            part[at, rt : rt + rp, :] = low_high(c[:rp], turned(c[rp:])).astype(BF16)
            db_k = db_own[k * rp : (k + 1) * rp]
            db[at] = db_k
            var = var + jnp.sum(step[at] * kt.astype(F32), axis=0, keepdims=True)
            var = var + jnp.sum(cols[at, 0:rp, :].astype(F32) * db_k, axis=0, keepdims=True)
        xs.append(x.astype(BF16))

    x = jnp.concatenate(xs, axis=0)
    var_rows = jnp.concatenate(split3(var) + [jnp.zeros((5, LANES), F32)], axis=0)
    for k, slot in enumerate(slots):
        y = jnp.bitwise_xor(lax.axis_index("y"), k)
        at = pl.ds(pl.multiple_of(y * LANES, LANES), LANES)
        p = [p[:, :, at].reshape(nj // 2 * rt, LANES) for p in (par_own, par_other)]
        partial = dot_t(jnp.concatenate(p, axis=0), x)
        rows = partial.shape[0]
        slot[0:rows, :] = partial[:, :LANES].astype(BF16)
        q = partial[:, LANES:]
        q = low_high(q[: rows // 2], turned(q[rows // 2 :]))
        slot[rows : rows + rows // 2 + 8, :] = jnp.concatenate([q, var_rows], axis=0).astype(BF16)


def sum_kernel(rt, rp, *refs):
    received, (db, part, out) = refs[:-3], refs[-3:]
    nj = out.shape[0]
    rows = nj * rp
    total = received[0][...].astype(F32)
    for one in received[1:]:
        total = total + one[...].astype(F32)
    q = total[rows : rows + rows // 2]
    q = jnp.concatenate([q, turned(q)], axis=0)
    first = rows + rows // 2
    var = total[first : first + 1] + total[first + 1 : first + 2] + total[first + 2 : first + 3]
    var_rows = []
    for top in split3(var):
        var_rows += [turned(top), top]
    var_rows = jnp.concatenate(var_rows + [jnp.zeros((2, LANES), F32)], axis=0)
    for j in range(nj):
        at = slice(j * rp, (j + 1) * rp)
        out[j, 0 : rt + rp, :] = part[j]
        kp = total[at] + db[j]
        out[j, rt + rp : rt + 3 * rp, :] = jnp.concatenate(
            [kp, low_high(q[at], var_rows)], axis=0
        ).astype(BF16)


def final_kernel(rt, rp, got, dinv, dvar, cross_par, sigma_par, kid_top, kid_par, variance):
    nj = got.shape[0]
    kids = dvar.shape[0]
    per_kid = nj // kids
    for j in range(nj):
        k, m = divmod(j, per_kid)
        at = slice(m * LANES, (m + 1) * LANES)
        kid_top[k, :, at] = got[j, 0:rt, :]
        kid_par[k, :, at] = got[j, rt + rp : rt + 2 * rp, :]
        v = got[j, rt + 2 * rp : rt + 3 * rp, :].astype(F32)
        low = v[0:1] + v[2:3] + v[4:5]
        high = v[1:2] + v[3:4] + v[5:6]
        variance[k : k + 1, at] = dvar[k : k + 1, at] + low_high(turned(low), high)
    for m in range(nj // 2):
        at = slice(m * LANES, (m + 1) * LANES)
        a = got[2 * m, rt : rt + rp, :].astype(F32)
        b = got[2 * m + 1, rt : rt + rp, :].astype(F32)
        cross_par[:, at] = jnp.concatenate(
            [low_high(a, turned(b)), low_high(turned(a), b)], axis=0
        ).astype(BF16)
        a = got[2 * m, rt + 2 * rp : rt + 3 * rp, :].astype(F32)
        b = got[2 * m + 1, rt + 2 * rp : rt + 3 * rp, :].astype(F32)
        sigma_par[:, at] = (dinv[:, at] + low_high(a, turned(b))).astype(BF16)


def device_part(
    sigma_top,
    panel_par,
    dinv_par,
    panel_kid_top,
    panel_kid_par,
    dvar_kid,
    mask_par,
    mask_kid_top,
    mask_kid_par,
):
    rt, wt = sigma_top.shape
    rp, w1 = dinv_par.shape
    kids, _, w2 = panel_kid_top.shape
    ny = lax.axis_size("y")
    nx = lax.axis_size("x")
    nj = lax.axis_size(XC)
    assert kids * w2 == nj * LANES and w1 == nj * HALF and wt == 2 * w1
    assert nx == 8 and rt == 2 * rp and nj * rp == LANES and ny * LANES == w1

    def fetching(kernel, outs, arrays):
        return call(
            kernel,
            outs,
            tuple(pltpu.with_memory_space_constraint(a, pltpu.HBM) for a in arrays),
            [pl.BlockSpec(memory_space=pltpu.HBM)] * len(arrays),
            [pltpu.VMEM(a.shape, a.dtype) for a in arrays]
            + [pltpu.SemaphoreType.DMA((len(arrays),))],
        )

    masks = (mask_par.T, mask_kid_top.transpose(0, 2, 1), mask_kid_par)
    slots, par_rows, rows = fetching(
        pack_kernel,
        [
            ((nj, 2 * rp + rt, LANES), BF16),
            ((rt, w1), BF16),
            ((2 * rt + rp, w1), BF16),
        ],
        (sigma_top, panel_par, dinv_par, panel_kid_top, panel_kid_par, *masks),
    )
    cols = exchanged(slots, XC)
    par_far = swapped(par_rows, "x", 4)
    far_rows = swapped(rows, "x", 4)
    (rows,) = call(copy_kernel, [(rows.shape, BF16)], (rows,))
    (tall_send,) = call(repeat_kernel, [((ny, nj, rp, LANES), BF16)], (cols,))
    (par_rows,) = call(
        stack_kernel,
        [((2, rt, w1), BF16)],
        (par_rows, par_far, tall_send),
        [VMEM, VMEM, pl.BlockSpec(memory_space=pl.ANY)],
    )
    par_far = swapped(par_rows, "x", 2)
    tall = exchanged(tall_send, "y")
    (rows,) = call(stack_kernel, [((2, 2 * rt + rp, w1), BF16)], (rows, far_rows))
    (par_rows,) = call(join_kernel, [((4, rt, w1), BF16)], (par_rows, par_far))
    par_own = jnp.concatenate([par_rows, swapped(par_rows, "x", 1)])
    par_other = swapped(par_own, "c", 1)
    rows_2 = swapped(rows, "x", 2)
    (rows,) = call(join_kernel, [((4, 2 * rt + rp, w1), BF16)], (rows, rows_2))
    near = jnp.concatenate([rows, swapped(rows, "x", 1)])
    far = swapped(near, "c", 1)

    def sized(kernel):
        return lambda *refs: kernel(rt, rp, *refs)

    rounded, step = call(
        sized(step_kernel),
        [((nj, rt + rp, LANES), BF16), ((nj, rt, LANES), F32)],
        (cols, tall, par_own, par_other),
    )
    steps = [rounded]
    for k in range(1, ny):
        steps.append(swapped(rounded, "y", k))
    rows4 = nj * rp + nj * rp // 2 + 8
    *partials, part, db = call(
        sized(main_kernel),
        [((rows4, LANES), BF16)] * ny
        + [((nj, rt + rp, LANES), BF16), ((nj, rp, LANES), F32)],
        (near, far, par_own, par_other, tall, cols, step, *steps),
        scratch=[
            pltpu.VMEM((ny, nj, rt, LANES), BF16),
            pltpu.VMEM((ny, nj, rp, LANES), F32),
        ],
    )
    for k in range(1, ny):
        partials[k] = swapped(partials[k], "y", k)
    (out,) = call(sized(sum_kernel), [((nj, rt + 3 * rp, LANES), BF16)], (*partials, db, part))
    got = exchanged(out, XC)
    return call(
        sized(final_kernel),
        [
            ((rt, w1), BF16),
            ((rp, w1), BF16),
            ((kids, rt, w2), BF16),
            ((kids, rp, w2), BF16),
            ((kids, w2), F32),
        ],
        (got, dinv_par, dvar_kid),
    )


def solution(mesh):
    finer = Mesh(mesh.devices.reshape(mesh.shape["parts"], 8, 8, 2), PARTS_ROW)
    return jax.shard_map(
        device_part,
        mesh=finer,
        in_specs=(
            P(PARTS_ROW, None),
            P(PARTS_ROW, None),
            P(PARTS_ROW, None),
            P("parts", ROW, None),
            P("parts", ROW, None),
            P("parts", None),
            P("parts", None),
            P("parts", None, None),
            P("parts", None, None),
        ),
        out_specs=(
            P(PARTS_ROW, None),
            P(PARTS_ROW, None),
            P("parts", ROW, None),
            P("parts", ROW, None),
            P("parts", None),
        ),
        check_vma=False,
    )
```
